32 devices in a mesh: groups: 2 (over y), seq: 4 (over z), exp: 2 (over x), tp: 2 (over core).
Axes of the slice: x: 2, y: 2, z: 4, core: 2. Of those that a mesh axis runs over, the one named last changes fastest.
Arguments:
- attn_query: bfloat16 [2048, 1152], P(('groups', 'seq'), ('exp', 'tp')), parts along dimension 0, may hold values from -6 to 6
- fresh_keys: bfloat16 [2048, 1152], P(('groups', 'seq'), ('exp', 'tp')), parts along dimension 0, may hold values from -6 to 6
- fresh_values: bfloat16 [2048, 1152], P(('groups', 'seq'), ('exp', 'tp')), parts along dimension 0, may hold values from -6 to 6
- stale_keys: bfloat16 [2048, 1152], P(('groups', 'seq'), ('exp', 'tp')), parts along dimension 0, may hold values from -6 to 6
- stale_values: bfloat16 [2048, 1152], P(('groups', 'seq'), ('exp', 'tp')), parts along dimension 0, may hold values from -6 to 6
- block_flags: int32 [16], P(('groups', 'seq')), parts along dimension 0, may hold values 0 or 1
- moe_tokens: bfloat16 [4096, 1152], P(('groups', 'seq', 'exp', 'tp')), parts along dimension 0, may hold values from -6 to 6
- expert_ids: int32 [4096, 2], P(('groups', 'seq', 'exp', 'tp')), parts along dimension 0, may hold values from 0 to 3, all different within a row; in each aligned block of 128 rows (0 to 127, 128 to 255, ...) at most 80 rows name the same one
- gate_weights: float32 [4096, 2], P(('groups', 'seq', 'exp', 'tp')), parts along dimension 0, may hold values from 0.25 to 1
- up_weight: bfloat16 [4, 1152, 4608], P('seq', None, ('exp', 'tp')), may hold values from -0.1875 to 0.1875
- up_bias: float32 [4, 4608], P('seq', ('exp', 'tp')), may hold values from -3 to 3
- down_weight: bfloat16 [4, 4608, 1152], P('seq', ('exp', 'tp')), may hold values from -0.09375 to 0.09375
- down_bias: float32 [4, 1152], P('seq'), may hold values from -2 to 2
Outputs:
- attn_out: bfloat16 [2048, 1152], P(('groups', 'seq'), ('exp', 'tp')), parts along dimension 0
- moe_out: bfloat16 [4096, 1152], P(('groups', 'seq', 'exp', 'tp')), parts along dimension 0
The draws below stay inside these ranges and needn't reach their ends.
There are 2 independent parts, one for each index of `groups`. The reference program is written for one: setup_inputs(seed, part) draws one part's arguments, and reference() takes and returns one part's arrays. A program takes and returns all parts, laid end to end along the dimension named above; an argument that names none is the same for every part. Nothing has to cross between parts.
Inputs may be any that keep to these rules, and one draw needn't show every extreme that they name: `expert_ids`: the 2 ids of a token differ. In the rows of one device no expert is named more than 80 times, and in every draw some expert is named exactly 80 times in some device's rows.
All inputs are finite; a program needn't handle non-finite values. No bound on the sum of `block_flags` on one device may be relied on, other than what follows from the above.
Results may differ from the reference program's by a relative error of at most 0.014.
Values may be sent and summed in bfloat16 or wider, within the bound.
A program may use at most 64 MiB of HBM per device.

```python
import math
import jax
import jax.numpy as jnp
import numpy as np
from jax import lax

D = 1152
HEADS = 16
HD = 72
FF = 4608
TOP = 2
EXPERTS = 4
BLK = 128
TOK_DEV = 128
SEQLEN = 1024
MOE_TOK = 2048
CAP = 80


def drawn(key):
    shape = (SEQLEN, HEADS * HD)
    query = jnp.clip(jax.random.normal(jax.random.fold_in(key, 101), shape, jnp.float32), -6.0, 6.0)
    keys_new = jnp.clip(jax.random.normal(jax.random.fold_in(key, 102), shape, jnp.float32), -6.0, 6.0)
    keys_old = jnp.clip(jax.random.normal(jax.random.fold_in(key, 103), shape, jnp.float32), -6.0, 6.0)
    return (query, keys_new, keys_old)


def draw_attn_query(key, part):
    return drawn(key)[0].astype(jnp.bfloat16)


def draw_fresh_keys(key, part):
    return drawn(key)[1].astype(jnp.bfloat16)


def draw_stale_keys(key, part):
    return drawn(key)[2].astype(jnp.bfloat16)


def place_ends(values, key, smallest, high):
    spot = [jax.random.randint(jax.random.fold_in(key, axis), (), 0, length) for axis, length in enumerate(values.shape)]
    main_axis = values.shape.index(max(values.shape))
    neighbour = spot[:main_axis] + [(spot[main_axis] + 1) % values.shape[main_axis]] + spot[main_axis + 1:]
    return values.at[tuple(spot)].set(smallest).at[tuple(neighbour)].set(high)


def steps_of(key, dims, shards, smallest, top_value):
    level = 1.0
    for dim, blocks in shards:
        heights = jax.random.uniform(jax.random.fold_in(jax.random.fold_in(key, 6), dim), (blocks,), jnp.float32, smallest / len(shards), top_value / len(shards))
        level = level * jnp.repeat(jnp.exp(heights), dims[dim] // blocks).reshape((-1,) + (1,) * (len(dims) - 1 - dim))
    return level


def assign_block(rng, own, number, rows, number_of, top, limit, lean):
    ranking = jax.random.permutation(rng, number_of)
    heavy_load, ordinary = portions_of(number_of, rows * top, limit, lean, True), portions_of(number_of, rows * top, limit, lean, False)
    places = jnp.arange(number_of)

    def named(tallies, offset_by):
        used = int((tallies > 0).sum())
        fixed = max(1, used // 4)
        passed = fixed + (places - fixed + offset_by * (used - fixed)) % max(1, number_of - fixed)
        return jnp.zeros((number_of,), jnp.int32).at[ranking[jnp.where(places < fixed, places, passed)]].set(jnp.asarray(tallies, jnp.int32))

    tallies = jnp.where(number % 4 == 0, named(heavy_load, number // 4), named(ordinary, number - number // 4 - 1))
    mixed = jax.random.permutation(jax.random.fold_in(own, 3), number_of)
    giver, sink = mixed[0:number_of // 2 * 2:2], mixed[1:number_of // 2 * 2:2]
    slack = jnp.minimum(tallies[giver] - 1, limit - tallies[sink]) // 2
    slack = jnp.where((giver == ranking[0]) | (sink == ranking[0]) | (tallies[sink] == 0), 0, jnp.maximum(slack, 0))
    passed = jax.random.randint(jax.random.fold_in(own, 4), (number_of // 2,), 0, 1 << 20) % (slack + 1)
    tallies = tallies.at[giver].add(-passed).at[sink].add(passed)
    labels = jnp.searchsorted(jnp.cumsum(tallies), jnp.arange(rows * top), side="right").astype(jnp.int32)
    listing = labels.reshape(top, rows).T
    listing = listing[jax.random.permutation(jax.random.fold_in(own, 1), rows)]
    offset_by = jax.random.randint(jax.random.fold_in(own, 2), (rows, 1), 0, top)
    return jnp.take_along_axis(listing, (jnp.arange(top)[None, :] + offset_by) % top, axis=1)


def portions_of(amount, total, limit, lean, full):
    weights = [(1 << 20) // math.isqrt(grade ** lean) + 1 for grade in range(1, amount + 1)]
    largest = limit if full else min(limit, max(-(-total // amount), total * weights[0] // sum(weights)))
    least = 1 if total - largest >= amount - 1 else 0
    given, spare = [largest] + [least] * (amount - 1), total - largest - least * (amount - 1)
    while spare > 0:
        free = [i for i in range(1, amount) if given[i] < largest] or [i for i in range(1, amount) if given[i] < limit]
        whole, budget = sum([weights[i] for i in free]), spare
        for i in free:
            more = min(limit - given[i], max(1, budget * weights[i] // whole), spare)
            given[i] = given[i] + more
            spare = spare - more
    return np.array(given)


def noise(key, dims, width, limit, cuts=(), kind=jnp.bfloat16):
    values = jax.random.normal(key, dims, jnp.float32) * width
    if len(cuts) > 0:
        values = steps_of(key, dims, cuts, -0.22, 0.18) * values
    return jnp.clip(values, min=-limit, max=limit).astype(kind)


def setup_inputs(seed: int = 0, part: int = 0) -> dict:
    streams_of = jax.random.split(jax.random.key(seed), 14)
    part_splits = jax.random.split(jax.random.fold_in(streams_of[13], part), 14)
    attn_query = draw_attn_query(jax.random.fold_in(jax.random.fold_in(streams_of[13], part), 71), part)
    fresh_keys = draw_fresh_keys(jax.random.fold_in(jax.random.fold_in(streams_of[13], part), 71), part)
    fresh_values = noise(part_splits[2], (SEQLEN, HEADS * HD), 1.0, 6.0, ((0, 4), (1, 4)))
    stale_keys = draw_stale_keys(jax.random.fold_in(jax.random.fold_in(streams_of[13], part), 71), part)
    stale_values = noise(part_splits[4], (SEQLEN, HEADS * HD), 1.0, 6.0, ((0, 4), (1, 4)))
    block_flags = place_ends((jax.random.randint(part_splits[5], (SEQLEN // BLK,), 0, 2) < 1).astype(jnp.int32), jax.random.fold_in(part_splits[5], 1), 0, 1)
    moe_tokens = noise(part_splits[6], (MOE_TOK, D), 1.0, 6.0, ((0, 16),))
    expert_ids_keys = jax.random.split(jax.random.fold_in(part_splits[7], 1), MOE_TOK // TOK_DEV)
    expert_ids_turns = jax.random.permutation(jax.random.fold_in(part_splits[7], 3), MOE_TOK // TOK_DEV)
    expert_ids = jax.vmap(lambda own, number: assign_block(jax.random.fold_in(part_splits[7], 2), own, number, TOK_DEV, EXPERTS, TOP, CAP, 2))(expert_ids_keys, expert_ids_turns).reshape((MOE_TOK, TOP))
    gate_weights = jnp.clip(jnp.exp(math.log(1.0) - 1.3862944 * jax.random.uniform(part_splits[8], (MOE_TOK, TOP), jnp.float32) ** steps_of(part_splits[8], (MOE_TOK, TOP), ((0, 16),), -0.2, 0.2)), 0.25, 1.0)
    up_weight = noise(streams_of[9], (EXPERTS, D, FF), D ** -0.5, 0.1875, ((0, 4), (2, 4)))
    up_bias = noise(streams_of[10], (EXPERTS, FF), 0.5, 3.0, ((0, 4), (1, 4)), jnp.float32)
    down_weight = noise(streams_of[11], (EXPERTS, FF, D), FF ** -0.5, 0.09375, ((0, 4), (1, 4)))
    down_bias = noise(streams_of[12], (EXPERTS, D), 0.3, 2.0, ((0, 4),), jnp.float32)
    return {"attn_query": attn_query, "fresh_keys": fresh_keys, "fresh_values": fresh_values, "stale_keys": stale_keys, "stale_values": stale_values, "block_flags": block_flags, "moe_tokens": moe_tokens, "expert_ids": expert_ids, "gate_weights": gate_weights, "up_weight": up_weight, "up_bias": up_bias, "down_weight": down_weight, "down_bias": down_bias}


def attention_part(attn_query, fresh_keys, fresh_values, stale_keys, stale_values, block_flags):
    row_flags = (jnp.repeat(block_flags, BLK) == 1)[:, None]
    keys = jnp.where(row_flags, fresh_keys, stale_keys)
    values = jnp.where(row_flags, fresh_values, stale_values)
    scale = 1.0 / math.sqrt(HD)
    query_block = math.gcd(SEQLEN, 1024)

    def head_fn(head):
        first = (head * HD).astype(jnp.int32)
        head_query = lax.dynamic_slice_in_dim(attn_query, first, HD, 1)
        head_keys = lax.dynamic_slice_in_dim(keys, first, HD, 1)
        head_values = lax.dynamic_slice_in_dim(values, first, HD, 1)

        def block_fn(index):
            lead = (index * query_block).astype(jnp.int32)
            rows = lax.dynamic_slice_in_dim(head_query, lead, query_block, 0)
            scores = jnp.dot(rows, head_keys.T, preferred_element_type=jnp.float32) * scale
            highest = lax.optimization_barrier(jnp.max(scores, axis=-1, keepdims=True))
            probs = jnp.exp(scores - highest)
            totals = lax.optimization_barrier(jnp.sum(probs, axis=-1, keepdims=True))
            mixed = jnp.dot(probs.astype(jnp.bfloat16), head_values, preferred_element_type=jnp.float32) / totals
            return mixed.astype(jnp.bfloat16)
        return lax.map(block_fn, jnp.arange(SEQLEN // query_block, dtype=jnp.int32))
    heads_out = lax.map(head_fn, jnp.arange(HEADS, dtype=jnp.int32))
    heads_out = heads_out.reshape(HEADS, SEQLEN, HD)
    return jnp.transpose(heads_out, (1, 0, 2)).reshape(SEQLEN, HEADS * HD)

def expert_part(moe_tokens, expert_ids, gate_weights, up_weight, up_bias, down_weight, down_bias):
    blocks = MOE_TOK // TOK_DEV
    block_ids = expert_ids.reshape(blocks, TOP * TOK_DEV)
    hits = (block_ids[:, :, None] == jnp.arange(EXPERTS, dtype=jnp.int32)[None, None, :]).astype(jnp.int32)
    before = jnp.cumsum(hits, axis=1) - hits
    place = lax.optimization_barrier(jnp.sum(before * hits, axis=-1)).reshape(-1).astype(jnp.int32)
    flat_expert = block_ids.reshape(-1).astype(jnp.int32)
    flat_block = jnp.repeat(jnp.arange(blocks, dtype=jnp.int32), TOP * TOK_DEV)
    repeated = jnp.repeat(moe_tokens, TOP, axis=0)
    buffer = jnp.zeros((EXPERTS, blocks, CAP, D), jnp.bfloat16)
    buffer = buffer.at[flat_expert, flat_block, place].set(repeated)

    def expert_fn(operands):
        slots, w_up, b_up, w_down, b_down = operands
        rows = slots.reshape(blocks * CAP, D)
        hidden = jax.nn.gelu(jnp.dot(rows, w_up, preferred_element_type=jnp.float32) + b_up[None, :]).astype(jnp.bfloat16)
        result = jnp.dot(hidden, w_down, preferred_element_type=jnp.float32) + b_down[None, :]
        return result.astype(jnp.bfloat16).reshape(blocks, CAP, D)
    expert_y = lax.map(expert_fn, (buffer, up_weight, up_bias, down_weight, down_bias))
    picked = expert_y[flat_expert, flat_block, place].reshape(MOE_TOK, TOP, D).astype(jnp.float32)
    combined = lax.optimization_barrier(jnp.sum(picked * gate_weights[:, :, None], axis=1))
    return combined.astype(jnp.bfloat16)

def reference(attn_query, fresh_keys, fresh_values, stale_keys, stale_values, block_flags, moe_tokens, expert_ids, gate_weights, up_weight, up_bias, down_weight, down_bias):
    attn_out = attention_part(attn_query, fresh_keys, fresh_values, stale_keys, stale_values, block_flags)
    moe_out = expert_part(moe_tokens, expert_ids, gate_weights, up_weight, up_bias, down_weight, down_bias)
    return (attn_out, moe_out)
```

```python
import functools
import math

import jax
import jax.numpy as jnp
from jax import lax
from jax.experimental import pallas as pl
from jax.experimental.pallas import tpu as pltpu
from jax.sharding import PartitionSpec as P

HD = 72
MESH = pl.DeviceIdType.MESH
F32 = jnp.float32
BF16 = jnp.bfloat16
VMEM_LIMIT = 40 * 1024 * 1024


def layer_kernel(
    sizes,
    q_ref, fresh_k, fresh_v, stale_k, stale_v, flags,
    tok_ref, ids_ref, gate_ref,
    up_hbm, upb_ref, down_hbm, downb_ref,
    attn_ref, moe_ref,
    up_v, down_v, place_v, disp, rows, tpin, xin, fin, ret, kv, keys_v, acc, turn,
    w_sem,
    z_send, z_recv, xf_send, xf_recv, tf_send, tf_recv,
    tr_send, tr_recv, xr_send, xr_recv, zr_send, zr_recv, kv_right, kv_left, kv_recv,
):
    S, X, capp = sizes
    s, x, c = lax.axis_index("seq"), lax.axis_index("exp"), lax.axis_index("tp")
    oc = 1 - c
    T, D = tok_ref.shape
    W, L = q_ref.shape
    heads = W // HD
    blk = L // flags.shape[0]

    up_copy = pltpu.make_async_copy(up_hbm.at[0], up_v, w_sem.at[0])
    down_copy = pltpu.make_async_copy(down_hbm.at[0], down_v, w_sem.at[1])
    up_copy.start()
    down_copy.start()

    def rdma(src, dst, ssem, rsem, where):
        return pltpu.make_async_remote_copy(
            src_ref=src, dst_ref=dst, send_sem=ssem, recv_sem=rsem,
            device_id=where, device_id_type=MESH,
        )

    def z_copy(e, slot):
        return rdma(disp.at[e], rows.at[slot, c, x], z_send.at[e], z_recv.at[slot], {"seq": e})

    def x_forward(src, to, origin):
        return rdma(
            rows.at[src, c, origin], rows.at[src, c, origin],
            xf_send.at[src, to], xf_recv.at[src, origin], {"exp": to},
        )

    def t_forward(src, origin, side):
        return rdma(
            rows.at[src, side, origin], rows.at[src, side, origin],
            tf_send.at[src, origin], tf_recv.at[src, origin], {"tp": oc},
        )

    def t_reduce(src):
        return rdma(rows.at[src, oc], tpin.at[src], tr_send.at[src], tr_recv.at[src], {"tp": oc})

    def x_reduce(src, to, origin):
        return rdma(
            rows.at[src, c, to], xin.at[src, origin],
            xr_send.at[src, to], xr_recv.at[src, origin], {"exp": to},
        )

    def z_return(src, slot):
        return rdma(fin.at[src], ret.at[slot], zr_send.at[src], zr_recv.at[slot], {"seq": src})

    def kv_copy(b, step):
        sems = kv_right if step > 0 else kv_left
        return rdma(kv.at[b], kv.at[b], sems.at[b], kv_recv.at[b], {"seq": s + step})

    def other_x(i):
        return lax.rem(x + i, X)

    def order(k):
        side = jnp.minimum(s, S - 1 - s)
        near = k // 2 + 1
        near = jnp.where(lax.rem(k, 2) == 0, near, -near)
        far = k - side + 1
        far = jnp.where(2 * s < S, far, -far)
        step = jnp.where(k < 2 * side, near, far)
        return s + jnp.where(k == S - 1, 0, step)

    barrier = pltpu.get_barrier_semaphore()
    for i in range(1, S):
        pl.semaphore_signal(barrier, inc=1, device_id={"seq": lax.rem(s + i, S)}, device_id_type=MESH)
    for i in range(1, X):
        pl.semaphore_signal(barrier, inc=1, device_id={"exp": other_x(i)}, device_id_type=MESH)
    pl.semaphore_signal(barrier, inc=1, device_id={"tp": oc}, device_id_type=MESH)

    expert = lax.broadcasted_iota(jnp.int32, (S, T), 0)
    named = (ids_ref[0:1, :] == expert) | (ids_ref[1:2, :] == expert)
    earlier = lax.broadcasted_iota(jnp.int32, (T, T), 0) < lax.broadcasted_iota(jnp.int32, (T, T), 1)
    place = jnp.dot(
        jnp.where(named, 1.0, 0.0).astype(BF16),
        jnp.where(earlier, 1.0, 0.0).astype(BF16),
        preferred_element_type=F32,
    )
    place_v[...] = jnp.where(named, place, -1.0)
    slot_rows = lax.broadcasted_iota(jnp.int32, (capp, T), 0).astype(F32)

    def slots_of(e):
        pick = jnp.where(place_v[pl.ds(e, 1), :] == slot_rows, 1.0, 0.0).astype(BF16)
        return jnp.dot(pick, tok_ref[...], preferred_element_type=F32).astype(BF16)

    def forward(src):
        for i in range(1, X):
            x_forward(src, other_x(i), x).start()
        t_forward(src, x, c).start()

    rows[s, c, x] = slots_of(s)
    pl.semaphore_wait(barrier, S - 1 + X - 1 + 1)
    forward(s)
    def dispatch(k):
        e = order(jnp.int32(k))
        disp[e] = slots_of(e)
        z_copy(e, s).start()

    for k in range(min(2, S - 1)):
        dispatch(k)
    for b in range(flags.shape[0]):
        fresh = flags[b] == 1
        part = pl.ds(b * blk, blk)
        kv[s, 0, :, part] = jnp.where(fresh, fresh_k[:, part], stale_k[:, part])
        kv[s, 1, :, part] = jnp.where(fresh, fresh_v[:, part], stale_v[:, part])

    def relay(step):
        low, high = s - (step - 1), s + (step - 1)

        @pl.when(low >= 0)
        def _():
            @pl.when(low < s)
            def _():
                kv_copy(low, 1).wait_recv()

            @pl.when(s + 1 < S)
            def _():
                kv_copy(low, 1).start()

        @pl.when(high < S)
        def _():
            @pl.when(high > s)
            def _():
                kv_copy(high, -1).wait_recv()

            @pl.when(s - 1 >= 0)
            def _():
                kv_copy(high, -1).start()

    relay(1)
    for k in range(2, S - 1):
        dispatch(k)
    nearest = order(jnp.int32(0))
    z_copy(nearest, nearest).wait_recv()
    forward(nearest)

    up_copy.wait()
    down_copy.wait()

    def finish(src):
        total = rows[src, c, x].astype(F32) + downb_ref[...]
        for i in range(1, X):
            x_reduce(src, other_x(i), other_x(i)).wait_recv()
            total = total + xin[src, other_x(i)].astype(F32)
        done = total.astype(BF16)
        fin[src] = done

    def finish_send(src):
        finish(src)

        @pl.when(src != s)
        def _():
            z_return(src, s).start()

        @pl.when(src == s)
        def _():
            ret[s] = fin[s]

    def chunk(k, unused):
        src = order(k)
        for i in range(1, X):
            x_forward(src, other_x(i), other_x(i)).wait_recv()
            t_forward(src, other_x(i), c).start()

        @pl.when(k + 1 < S - 1)
        def _():
            nxt = order(k + 1)
            z_copy(nxt, nxt).wait_recv()
            forward(nxt)

        for i in range(X):
            t_forward(src, other_x(i), oc).wait_recv()
        for i in range(1, X):
            x_forward(src, other_x(i), x).wait_send()
        for i in range(X):
            t_forward(src, other_x(i), c).wait_send()

        block = rows[src].reshape(2 * X * capp, D)
        hidden = jnp.dot(block, up_v[...], preferred_element_type=F32) + upb_ref[...]
        hidden = jax.nn.gelu(hidden).astype(BF16)
        result = jnp.dot(hidden, down_v[...], preferred_element_type=F32).astype(BF16)
        rows[src] = result.reshape(2, X, capp, D)
        t_reduce(src).start()

        @pl.when(k >= 1)
        def _():
            finish_send(order(k - 1))

        @pl.when(k == 0)
        def _():
            relay(2)

        @pl.when((k >= 2) & (k < S - 1))
        def _():
            relay(k + 1)

        t_reduce(src).wait_recv()
        for i in range(X):
            to = other_x(i)
            rows[src, c, to] = (rows[src, c, to].astype(F32) + tpin[src, to].astype(F32)).astype(BF16)
            if i > 0:
                x_reduce(src, to, x).start()
        return unused

    lax.fori_loop(0, S, chunk, jnp.int32(0))

    relay(S)

    for i in range(S):
        keys_v[pl.ds(i * L, L), :] = kv[i, 0].T
    scale = 1.0 / math.sqrt(HD)
    channel = lax.broadcasted_iota(jnp.int32, (W, L), 0)

    def head(h, unused):
        mine = (channel >= h * HD) & (channel < (h + 1) * HD)
        query = jnp.where(mine, q_ref[...].astype(F32), 0.0).astype(BF16)
        scores = jnp.dot(keys_v[...], query, preferred_element_type=F32) * scale
        probs = jnp.exp(scores - jnp.max(scores, axis=0, keepdims=True))
        total = jnp.sum(probs, axis=0, keepdims=True)
        weights = probs.astype(BF16)
        mixed = jnp.zeros((W, L), F32)
        for i in range(S):
            mixed += jnp.dot(kv[i, 1], weights[i * L : (i + 1) * L], preferred_element_type=F32)
        acc[...] = jnp.where(mine, mixed / total, acc[...])
        return unused

    acc[...] = jnp.zeros_like(acc)
    lax.fori_loop(0, heads, head, jnp.int32(0))
    attn_ref[...] = acc[...].astype(BF16)
    finish_send(s)

    base = jnp.where(named, place, 0.0) + (expert * capp).astype(F32)
    turn[...] = jnp.zeros_like(turn)
    for j in range(2):
        hit = ids_ref[j : j + 1, :] == expert
        turn[j : j + 1, :] = jnp.sum(jnp.where(hit, base, 0.0), axis=0, keepdims=True)
        turn[2 + j : 3 + j, :] = gate_ref[j : j + 1, :]
    turned = turn[...].T
    slot_lane = lax.broadcasted_iota(jnp.int32, (T, S * capp), 1).astype(F32)
    picks = [jnp.where(turned[:, j : j + 1] == slot_lane, 1.0, 0.0).astype(BF16) for j in range(2)]
    for i in range(1, S):
        z_return(s, lax.rem(s + i, S)).wait_recv()
    everything = ret[...].reshape(S * capp, D)
    moe_ref[...] = (
        jnp.dot(picks[0], everything, preferred_element_type=F32) * turned[:, 2:3]
        + jnp.dot(picks[1], everything, preferred_element_type=F32) * turned[:, 3:4]
    ).astype(BF16)

    def drain(i, unused):
        to = lax.rem(s + i, S)
        z_copy(to, s).wait_send()
        z_return(to, s).wait_send()
        return unused

    lax.fori_loop(1, S, drain, jnp.int32(0))

    def drain_chunk(i, unused):
        t_reduce(i).wait_send()
        for j in range(1, X):
            x_reduce(i, other_x(j), x).wait_send()

        @pl.when((i <= s) & (s + 1 < S))
        def _():
            kv_copy(i, 1).wait_send()

        @pl.when((i >= s) & (s - 1 >= 0))
        def _():
            kv_copy(i, -1).wait_send()

        return unused

    lax.fori_loop(0, S, drain_chunk, jnp.int32(0))


def fast_kernel(
    sizes,
    q_hbm, fk_hbm, fv_hbm, sk_hbm, sv_hbm, flags_hbm, tok_hbm, ids_hbm, gate_hbm,
    up_hbm, upb_hbm, down_hbm, downb_hbm,
    attn_ref, moe_ref,
    q_v, fresh_k, fresh_v, stale_k, stale_v, flags, tok_v, ids_v, gate_v,
    up_v, upb_v, down_v, downb_v,
    disp, rows, outs, tpin, xin, fin, ret, kv, keys_v, acc, moe, turn,
    in_sem,
    z_send, z_recv, xf_send, xf_recv, tf_send, tf_recv,
    tr_send, tr_recv, xr_send, xr_recv, zr_send, zr_recv, kv_right, kv_left, kv_recv,
):
    S, X, capp = sizes
    s, x, c = lax.axis_index("seq"), lax.axis_index("exp"), lax.axis_index("tp")
    oc, ox = 1 - c, 1 - x
    T, D = tok_v.shape
    W, L = q_v.shape
    heads = W // HD
    blocks = flags.shape[0]
    blk = L // blocks

    barrier = pltpu.get_barrier_semaphore()
    for i in range(1, S):
        pl.semaphore_signal(barrier, inc=1, device_id={"seq": lax.rem(s + i, S)}, device_id_type=MESH)
    pl.semaphore_signal(barrier, inc=1, device_id={"exp": ox}, device_id_type=MESH)
    pl.semaphore_signal(barrier, inc=1, device_id={"tp": oc}, device_id_type=MESH)

    pairs = (
        (ids_hbm, ids_v), (tok_hbm, tok_v), (flags_hbm, flags),
        (fk_hbm, fresh_k), (sk_hbm, stale_k), (fv_hbm, fresh_v), (sv_hbm, stale_v),
        (up_hbm.at[0], up_v), (upb_hbm, upb_v), (down_hbm.at[0], down_v), (downb_hbm, downb_v),
        (q_hbm, q_v), (gate_hbm, gate_v),
    )
    loads = [pltpu.make_async_copy(a, b, in_sem.at[i]) for i, (a, b) in enumerate(pairs)]
    for load in loads:
        load.start()

    def rdma(src, dst, ssem, rsem, where):
        return pltpu.make_async_remote_copy(
            src_ref=src, dst_ref=dst, send_sem=ssem, recv_sem=rsem,
            device_id=where, device_id_type=MESH,
        )

    def z_copy(e, slot):
        return rdma(disp.at[e], rows.at[slot, x, c], z_send.at[e], z_recv.at[slot], {"seq": e})

    def x_forward(src, origin):
        return rdma(
            rows.at[src, origin, c], rows.at[src, origin, c],
            xf_send.at[src], xf_recv.at[src], {"exp": ox},
        )

    def t_forward(src, origin, side):
        return rdma(
            rows.at[src, origin, side], rows.at[src, origin, side],
            tf_send.at[src, origin], tf_recv.at[src, origin], {"tp": oc},
        )

    def t_reduce(src, origin):
        return rdma(
            outs.at[src, origin, oc], tpin.at[src, origin],
            tr_send.at[src, origin], tr_recv.at[src, origin], {"tp": oc},
        )

    def x_reduce(src):
        return rdma(outs.at[src, ox, c], xin.at[src], xr_send.at[src], xr_recv.at[src], {"exp": ox})

    def z_return(src, slot):
        return rdma(fin.at[src], ret.at[slot], zr_send.at[src], zr_recv.at[slot], {"seq": src})

    def kv_copy(b, part, step):
        sems = kv_right if step > 0 else kv_left
        return rdma(
            kv.at[b, part], kv.at[b, part], sems.at[b, part], kv_recv.at[b, part], {"seq": s + step}
        )

    def mirrored(end, inner):
        near = jnp.where((s == 0) | (s == S - 1), end, inner)
        return jnp.where(2 * s < S, near, S - 1 - near)

    targets = [mirrored(a, b) for a, b in ((S - 1, 2), (1, 0), (2, S - 1))]
    order = [s] + [mirrored(a, b) for a, b in ((1, 2), (S - 1, 0), (2, S - 1))]

    loads[0].wait()
    loads[1].wait()
    expert = lax.broadcasted_iota(jnp.int32, (S, T), 0)
    named = (ids_v[0:1, :] == expert) | (ids_v[1:2, :] == expert)
    earlier = lax.broadcasted_iota(jnp.int32, (T, T), 0) < lax.broadcasted_iota(jnp.int32, (T, T), 1)
    place = jnp.dot(
        jnp.where(named, 1.0, 0.0).astype(BF16),
        jnp.where(earlier, 1.0, 0.0).astype(BF16),
        preferred_element_type=F32,
    )
    slotted = jnp.where(named, place, -1.0)
    slot_rows = lax.broadcasted_iota(jnp.int32, (capp, T), 0).astype(F32)
    for e in range(S):
        pick = jnp.where(slotted[e : e + 1, :] == slot_rows, 1.0, 0.0).astype(BF16)
        disp[e] = jnp.dot(pick, tok_v[...], preferred_element_type=F32).astype(BF16)
    rows[s, x, c] = disp[s]
    for load in loads[2:7]:
        load.wait()
    for b in range(blocks):
        fresh = flags[b] == 1
        part = pl.ds(b * blk, blk)
        kv[s, 0, :, part] = jnp.where(fresh, fresh_k[:, part], stale_k[:, part])
        kv[s, 1, :, part] = jnp.where(fresh, fresh_v[:, part], stale_v[:, part])

    pl.semaphore_wait(barrier, S - 1 + 1 + 1)

    def forward(src):
        x_forward(src, x).start()
        t_forward(src, x, c).start()

    def arrive(src):
        z_copy(src, src).wait_recv()
        forward(src)

    for e in targets:
        z_copy(e, s).start()
    forward(s)

    def relay(step, part):
        low, high = s - (step - 1), s + (step - 1)

        @pl.when(low >= 0)
        def _():
            @pl.when(low < s)
            def _():
                kv_copy(low, part, 1).wait_recv()

            @pl.when(s + 1 < S)
            def _():
                kv_copy(low, part, 1).start()

        @pl.when(high < S)
        def _():
            @pl.when(high > s)
            def _():
                kv_copy(high, part, -1).wait_recv()

            @pl.when(s - 1 >= 0)
            def _():
                kv_copy(high, part, -1).start()

    relay(1, 0)
    relay(1, 1)
    for load in loads[7:]:
        load.wait()

    def mlp(src, origin):
        block = rows[src, origin].reshape(2 * capp, D)
        hidden = jnp.dot(block, up_v[...], preferred_element_type=F32) + upb_v[...]
        hidden = jax.nn.gelu(hidden).astype(BF16)
        result = jnp.dot(hidden, down_v[...], preferred_element_type=F32).astype(BF16)
        outs[src, origin] = result.reshape(2, capp, D)
        t_reduce(src, origin).start()

    def mine(src):
        t_forward(src, x, oc).wait_recv()
        mlp(src, x)

    def crossed(src):
        x_forward(src, ox).wait_recv()
        t_forward(src, ox, c).start()

    def other(src):
        t_forward(src, ox, oc).wait_recv()
        mlp(src, ox)

    def reduce(src):
        t_reduce(src, ox).wait_recv()
        outs[src, ox, c] = (outs[src, ox, c].astype(F32) + tpin[src, ox].astype(F32)).astype(BF16)
        x_reduce(src).start()

    def finish(src):
        t_reduce(src, x).wait_recv()
        total = outs[src, x, c].astype(F32) + tpin[src, x].astype(F32) + downb_v[...]
        x_reduce(src).wait_recv()
        return (total + xin[src].astype(F32)).astype(BF16)

    def finish_send(src):
        fin[src] = finish(src)
        z_return(src, s).start()

    o0, o1, o2, o3 = order
    mine(o0)
    turn[...] = jnp.zeros_like(turn)
    for i, e in enumerate(order):
        hit = [ids_v[j : j + 1, :] == e for j in range(2)]
        spot = jnp.sum(jnp.where(expert == e, place, 0.0), axis=0, keepdims=True)
        turn[i : i + 1, :] = jnp.where(hit[0] | hit[1], spot, -1.0)
        turn[S + i : S + i + 1, :] = sum(
            jnp.where(hit[j], gate_v[j : j + 1, :], 0.0) for j in range(2)
        )
    turned = turn[...].T
    slot_lane = lax.broadcasted_iota(jnp.int32, (T, capp), 1).astype(F32)
    arrive(o1)
    crossed(o0)
    mine(o1)
    other(o0)
    arrive(o2)
    mine(o2)
    crossed(o1)
    arrive(o3)
    other(o1)
    mine(o3)
    reduce(o1)
    crossed(o2)
    other(o2)
    relay(2, 0)
    reduce(o2)
    relay(2, 1)
    crossed(o3)
    other(o3)
    reduce(o3)
    reduce(o0)
    relay(3, 0)
    finish_send(o1)
    relay(3, 1)
    finish_send(o2)
    finish_send(o3)
    relay(4, 0)
    relay(4, 1)

    for i in range(S):
        keys_v[pl.ds(i * L, L), :] = kv[i, 0].T
    scale = 1.0 / math.sqrt(HD)
    channel = lax.broadcasted_iota(jnp.int32, (W, L), 0)

    def head(h, unused):
        mask = (channel >= h * HD) & (channel < (h + 1) * HD)
        query = jnp.where(mask, q_v[...].astype(F32), 0.0).astype(BF16)
        scores = jnp.dot(keys_v[...], query, preferred_element_type=F32) * scale
        probs = jnp.exp(scores - jnp.max(scores, axis=0, keepdims=True))
        total = jnp.sum(probs, axis=0, keepdims=True)
        weights = probs.astype(BF16)
        mixed = jnp.zeros((W, L), F32)
        for i in range(S):
            mixed += jnp.dot(kv[i, 1], weights[i * L : (i + 1) * L], preferred_element_type=F32)
        acc[...] = jnp.where(mask, mixed / total, acc[...])
        return unused

    acc[...] = jnp.zeros_like(acc)
    lax.fori_loop(0, heads, head, jnp.int32(0))
    attn_ref[...] = acc[...].astype(BF16)

    def combine(i, values):
        pick = jnp.where(turned[:, i : i + 1] == slot_lane, 1.0, 0.0).astype(BF16)
        return jnp.dot(pick, values, preferred_element_type=F32) * turned[:, S + i : S + i + 1]

    moe[...] = combine(0, finish(s))
    for i in range(1, S - 1):
        z_return(s, order[i]).wait_recv()
        moe[...] += combine(i, ret[order[i]])
    z_return(s, order[S - 1]).wait_recv()
    moe_ref[...] = (moe[...] + combine(S - 1, ret[order[S - 1]])).astype(BF16)

    def drain(i, unused):
        to = lax.rem(s + i, S)
        z_copy(to, s).wait_send()
        z_return(to, s).wait_send()
        return unused

    lax.fori_loop(1, S, drain, jnp.int32(0))

    def drain_chunk(i, unused):
        x_forward(i, x).wait_send()
        x_reduce(i).wait_send()
        for origin in range(X):
            t_forward(i, origin, c).wait_send()
            t_reduce(i, origin).wait_send()
        for part in range(2):

            @pl.when((i <= s) & (s + 1 < S))
            def _():
                kv_copy(i, part, 1).wait_send()

            @pl.when((i >= s) & (s - 1 >= 0))
            def _():
                kv_copy(i, part, -1).wait_send()

        return unused

    lax.fori_loop(0, S, drain_chunk, jnp.int32(0))


def fast_call(S, X, capp, args):
    q, tok, up, flags = args[0], args[6], args[9], args[5]
    width, length = q.shape
    tokens, D = tok.shape
    hidden = up.shape[2]
    hbm = pl.BlockSpec(memory_space=pltpu.HBM)
    vmem = pl.BlockSpec(memory_space=pltpu.VMEM)
    dma = pltpu.SemaphoreType.DMA
    half = pltpu.VMEM((width, length), BF16)
    slots = pltpu.VMEM((S, capp, D), BF16)
    return pl.pallas_call(
        functools.partial(fast_kernel, (S, X, capp)),
        out_shape=(
            jax.ShapeDtypeStruct((width, length), BF16),
            jax.ShapeDtypeStruct((tokens, D), BF16),
        ),
        in_specs=[hbm] * 13,
        out_specs=(vmem, vmem),
        scratch_shapes=[
            half, half, half, half, half,
            pltpu.SMEM(flags.shape, jnp.int32),
            pltpu.VMEM((tokens, D), BF16),
            pltpu.VMEM((2, tokens), jnp.int32),
            pltpu.VMEM((2, tokens), F32),
            pltpu.VMEM((D, hidden), BF16),
            pltpu.VMEM((1, hidden), F32),
            pltpu.VMEM((hidden, D), BF16),
            pltpu.VMEM((1, D), F32),
            slots,
            pltpu.VMEM((S, X, 2, capp, D), BF16),
            pltpu.VMEM((S, X, 2, capp, D), BF16),
            pltpu.VMEM((S, X, capp, D), BF16),
            slots, slots, slots,
            pltpu.VMEM((S, 2, width, length), BF16),
            pltpu.VMEM((S * length, width), BF16),
            pltpu.VMEM((width, length), F32),
            pltpu.VMEM((tokens, D), F32),
            pltpu.VMEM((128, tokens), F32),
            dma((13,)),
            dma((S,)), dma((S,)), dma((S,)), dma((S,)), dma((S, X)), dma((S, X)),
            dma((S, X)), dma((S, X)), dma((S,)), dma((S,)), dma((S,)), dma((S,)),
            dma((S, 2)), dma((S, 2)), dma((S, 2)),
        ],
        compiler_params=pltpu.CompilerParams(
            collective_id=0, has_side_effects=True, vmem_limit_bytes=VMEM_LIMIT
        ),
    )(*[pltpu.with_memory_space_constraint(a, pltpu.HBM) for a in args])


def local(
    attn_query, fresh_keys, fresh_values, stale_keys, stale_values, block_flags,
    moe_tokens, expert_ids, gate_weights, up_weight, up_bias, down_weight, down_bias,
):
    S, X = lax.axis_size("seq"), lax.axis_size("exp")
    assert lax.axis_size("tp") == 2 and up_weight.shape[0] == 1
    tokens, D = moe_tokens.shape
    length, width = attn_query.shape
    hidden = up_weight.shape[2]
    cap = 5 * tokens // (2 * S)
    capp = -(-cap // 16) * 16
    if (S, X) == (4, 2):
        attn_out, moe_out = fast_call(S, X, capp, (
            attn_query.T, fresh_keys.T, fresh_values.T, stale_keys.T, stale_values.T, block_flags,
            moe_tokens, expert_ids.T, gate_weights.T,
            up_weight, up_bias, down_weight, down_bias,
        ))
        return attn_out.T, moe_out
    vmem = pl.BlockSpec(memory_space=pltpu.VMEM)
    smem = pl.BlockSpec(memory_space=pltpu.SMEM)
    hbm = pl.BlockSpec(memory_space=pl.ANY)
    dma = pltpu.SemaphoreType.DMA
    attn_out, moe_out = pl.pallas_call(
        functools.partial(layer_kernel, (S, X, capp)),
        out_shape=(
            jax.ShapeDtypeStruct((width, length), BF16),
            jax.ShapeDtypeStruct((tokens, D), BF16),
        ),
        in_specs=[vmem] * 5 + [smem] + [vmem] * 3 + [hbm, vmem, hbm, vmem],
        out_specs=(vmem, vmem),
        scratch_shapes=[
            pltpu.VMEM((D, hidden), BF16),
            pltpu.VMEM((hidden, D), BF16),
            pltpu.VMEM((S, tokens), F32),
            pltpu.VMEM((S, capp, D), BF16),
            pltpu.VMEM((S, 2, X, capp, D), BF16),
            pltpu.VMEM((S, X, capp, D), BF16),
            pltpu.VMEM((S, X, capp, D), BF16),
            pltpu.VMEM((S, capp, D), BF16),
            pltpu.VMEM((S, capp, D), BF16),
            pltpu.VMEM((S, 2, width, length), BF16),
            pltpu.VMEM((S * length, width), BF16),
            pltpu.VMEM((width, length), F32),
            pltpu.VMEM((128, tokens), F32),
            dma((2,)),
            dma((S,)), dma((S,)), dma((S, X)), dma((S, X)), dma((S, X)), dma((S, X)),
            dma((S,)), dma((S,)), dma((S, X)), dma((S, X)), dma((S,)), dma((S,)),
            dma((S,)), dma((S,)), dma((S,)),
        ],
        compiler_params=pltpu.CompilerParams(
            collective_id=0, has_side_effects=True, vmem_limit_bytes=67043328
        ),
    )(
        attn_query.T, fresh_keys.T, fresh_values.T, stale_keys.T, stale_values.T, block_flags,
        moe_tokens, expert_ids.T, gate_weights.T,
        up_weight, up_bias, down_weight, down_bias,
    )
    return attn_out.T, moe_out


def solution(mesh):
    in_specs = (
        P(("groups", "seq"), ("exp", "tp")),
        P(("groups", "seq"), ("exp", "tp")),
        P(("groups", "seq"), ("exp", "tp")),
        P(("groups", "seq"), ("exp", "tp")),
        P(("groups", "seq"), ("exp", "tp")),
        P(("groups", "seq")),
        P(("groups", "seq", "exp", "tp"), None),
        P(("groups", "seq", "exp", "tp"), None),
        P(("groups", "seq", "exp", "tp"), None),
        P("seq", None, ("exp", "tp")),
        P("seq", ("exp", "tp")),
        P("seq", ("exp", "tp"), None),
        P("seq", None),
    )
    out_specs = (P(("groups", "seq"), ("exp", "tp")), P(("groups", "seq", "exp", "tp"), None))
    return jax.shard_map(local, mesh=mesh, in_specs=in_specs, out_specs=out_specs, check_vma=False)
```

```python
import functools
import math

import jax
import jax.numpy as jnp
from jax import lax
from jax.experimental import pallas as pl
from jax.experimental.pallas import tpu as pltpu
from jax.sharding import PartitionSpec as P

HD = 72
MESH = pl.DeviceIdType.MESH
F32 = jnp.float32
BF16 = jnp.bfloat16
VMEM_LIMIT = 40 * 1024 * 1024


def layer_kernel(
    sizes,
    q_ref, fresh_k, fresh_v, stale_k, stale_v, flags,
    tok_ref, ids_ref, gate_ref,
    up_hbm, upb_ref, down_hbm, downb_ref,
    attn_ref, moe_ref,
    up_v, down_v, place_v, disp, rows, tpin, xin, fin, ret, kv, keys_v, acc, turn,
    w_sem,
    z_send, z_recv, xf_send, xf_recv, tf_send, tf_recv,
    tr_send, tr_recv, xr_send, xr_recv, zr_send, zr_recv, kv_right, kv_left, kv_recv,
):
    S, X, capp = sizes
    s, x, c = lax.axis_index("seq"), lax.axis_index("exp"), lax.axis_index("tp")
    oc = 1 - c
    T, D = tok_ref.shape
    W, L = q_ref.shape
    heads = W // HD
    blk = L // flags.shape[0]

    up_copy = pltpu.make_async_copy(up_hbm.at[0], up_v, w_sem.at[0])
    down_copy = pltpu.make_async_copy(down_hbm.at[0], down_v, w_sem.at[1])
    up_copy.start()
    down_copy.start()

    def rdma(src, dst, ssem, rsem, where):
        return pltpu.make_async_remote_copy(
            src_ref=src, dst_ref=dst, send_sem=ssem, recv_sem=rsem,
            device_id=where, device_id_type=MESH,
        )

    def z_copy(e, slot):
        return rdma(disp.at[e], rows.at[slot, c, x], z_send.at[e], z_recv.at[slot], {"seq": e})

    def x_forward(src, to, origin):
        return rdma(
            rows.at[src, c, origin], rows.at[src, c, origin],
            xf_send.at[src, to], xf_recv.at[src, origin], {"exp": to},
        )

    def t_forward(src, origin, side):
        return rdma(
            rows.at[src, side, origin], rows.at[src, side, origin],
            tf_send.at[src, origin], tf_recv.at[src, origin], {"tp": oc},
        )

    def t_reduce(src):
        return rdma(rows.at[src, oc], tpin.at[src], tr_send.at[src], tr_recv.at[src], {"tp": oc})

    def x_reduce(src, to, origin):
        return rdma(
            rows.at[src, c, to], xin.at[src, origin],
            xr_send.at[src, to], xr_recv.at[src, origin], {"exp": to},
        )

    def z_return(src, slot):
        return rdma(fin.at[src], ret.at[slot], zr_send.at[src], zr_recv.at[slot], {"seq": src})

    def kv_copy(b, step):
        sems = kv_right if step > 0 else kv_left
        return rdma(kv.at[b], kv.at[b], sems.at[b], kv_recv.at[b], {"seq": s + step})

    def other_x(i):
        return lax.rem(x + i, X)

    def order(k):
        side = jnp.minimum(s, S - 1 - s)
        near = k // 2 + 1
        near = jnp.where(lax.rem(k, 2) == 0, near, -near)
        far = k - side + 1
        far = jnp.where(2 * s < S, far, -far)
        step = jnp.where(k < 2 * side, near, far)
        return s + jnp.where(k == S - 1, 0, step)

    barrier = pltpu.get_barrier_semaphore()
    for i in range(1, S):
        pl.semaphore_signal(barrier, inc=1, device_id={"seq": lax.rem(s + i, S)}, device_id_type=MESH)
    for i in range(1, X):
        pl.semaphore_signal(barrier, inc=1, device_id={"exp": other_x(i)}, device_id_type=MESH)
    pl.semaphore_signal(barrier, inc=1, device_id={"tp": oc}, device_id_type=MESH)

    expert = lax.broadcasted_iota(jnp.int32, (S, T), 0)
    named = (ids_ref[0:1, :] == expert) | (ids_ref[1:2, :] == expert)
    earlier = lax.broadcasted_iota(jnp.int32, (T, T), 0) < lax.broadcasted_iota(jnp.int32, (T, T), 1)
    place = jnp.dot(
        jnp.where(named, 1.0, 0.0).astype(BF16),
        jnp.where(earlier, 1.0, 0.0).astype(BF16),
        preferred_element_type=F32,
    )
    place_v[...] = jnp.where(named, place, -1.0)
    slot_rows = lax.broadcasted_iota(jnp.int32, (capp, T), 0).astype(F32)

    def slots_of(e):
        pick = jnp.where(place_v[pl.ds(e, 1), :] == slot_rows, 1.0, 0.0).astype(BF16)
        return jnp.dot(pick, tok_ref[...], preferred_element_type=F32).astype(BF16)

    def forward(src):
        for i in range(1, X):
            x_forward(src, other_x(i), x).start()
        t_forward(src, x, c).start()

    rows[s, c, x] = slots_of(s)
    pl.semaphore_wait(barrier, S - 1 + X - 1 + 1)
    forward(s)
    def dispatch(k):
        e = order(jnp.int32(k))
        disp[e] = slots_of(e)
        z_copy(e, s).start()

    for k in range(min(2, S - 1)):
        dispatch(k)
    for b in range(flags.shape[0]):
        fresh = flags[b] == 1
        part = pl.ds(b * blk, blk)
        kv[s, 0, :, part] = jnp.where(fresh, fresh_k[:, part], stale_k[:, part])
        kv[s, 1, :, part] = jnp.where(fresh, fresh_v[:, part], stale_v[:, part])

    def relay(step):
        low, high = s - (step - 1), s + (step - 1)

        @pl.when(low >= 0)
        def _():
            @pl.when(low < s)
            def _():
                kv_copy(low, 1).wait_recv()

            @pl.when(s + 1 < S)
            def _():
                kv_copy(low, 1).start()

        @pl.when(high < S)
        def _():
            @pl.when(high > s)
            def _():
                kv_copy(high, -1).wait_recv()

            @pl.when(s - 1 >= 0)
            def _():
                kv_copy(high, -1).start()

    relay(1)
    for k in range(2, S - 1):
        dispatch(k)
    nearest = order(jnp.int32(0))
    z_copy(nearest, nearest).wait_recv()
    forward(nearest)

    up_copy.wait()
    down_copy.wait()

    def finish(src):
        total = rows[src, c, x].astype(F32) + downb_ref[...]
        for i in range(1, X):
            x_reduce(src, other_x(i), other_x(i)).wait_recv()
            total = total + xin[src, other_x(i)].astype(F32)
        done = total.astype(BF16)
        fin[src] = done

    def finish_send(src):
        finish(src)

        @pl.when(src != s)
        def _():
            z_return(src, s).start()

        @pl.when(src == s)
        def _():
            ret[s] = fin[s]

    def chunk(k, unused):
        src = order(k)
        for i in range(1, X):
            x_forward(src, other_x(i), other_x(i)).wait_recv()
            t_forward(src, other_x(i), c).start()

        @pl.when(k + 1 < S - 1)
        def _():
            nxt = order(k + 1)
            z_copy(nxt, nxt).wait_recv()
            forward(nxt)

        for i in range(X):
            t_forward(src, other_x(i), oc).wait_recv()
        for i in range(1, X):
            x_forward(src, other_x(i), x).wait_send()
        for i in range(X):
            t_forward(src, other_x(i), c).wait_send()

        block = rows[src].reshape(2 * X * capp, D)
        hidden = jnp.dot(block, up_v[...], preferred_element_type=F32) + upb_ref[...]
        hidden = jax.nn.gelu(hidden).astype(BF16)
        result = jnp.dot(hidden, down_v[...], preferred_element_type=F32).astype(BF16)
        rows[src] = result.reshape(2, X, capp, D)
        t_reduce(src).start()

        @pl.when(k >= 1)
        def _():
            finish_send(order(k - 1))

        @pl.when(k == 0)
        def _():
            relay(2)

        @pl.when((k >= 2) & (k < S - 1))
        def _():
            relay(k + 1)

        t_reduce(src).wait_recv()
        for i in range(X):
            to = other_x(i)
            rows[src, c, to] = (rows[src, c, to].astype(F32) + tpin[src, to].astype(F32)).astype(BF16)
            if i > 0:
                x_reduce(src, to, x).start()
        return unused

    lax.fori_loop(0, S, chunk, jnp.int32(0))

    relay(S)

    for i in range(S):
        keys_v[pl.ds(i * L, L), :] = kv[i, 0].T
    scale = 1.0 / math.sqrt(HD)
    channel = lax.broadcasted_iota(jnp.int32, (W, L), 0)

    def head(h, unused):
        mine = (channel >= h * HD) & (channel < (h + 1) * HD)
        query = jnp.where(mine, q_ref[...].astype(F32), 0.0).astype(BF16)
        scores = jnp.dot(keys_v[...], query, preferred_element_type=F32) * scale
        probs = jnp.exp(scores - jnp.max(scores, axis=0, keepdims=True))
        total = jnp.sum(probs, axis=0, keepdims=True)
        weights = probs.astype(BF16)
        mixed = jnp.zeros((W, L), F32)
        for i in range(S):
            mixed += jnp.dot(kv[i, 1], weights[i * L : (i + 1) * L], preferred_element_type=F32)
        acc[...] = jnp.where(mine, mixed / total, acc[...])
        return unused

    acc[...] = jnp.zeros_like(acc)
    lax.fori_loop(0, heads, head, jnp.int32(0))
    attn_ref[...] = acc[...].astype(BF16)
    finish_send(s)

    base = jnp.where(named, place, 0.0) + (expert * capp).astype(F32)
    turn[...] = jnp.zeros_like(turn)
    for j in range(2):
        hit = ids_ref[j : j + 1, :] == expert
        turn[j : j + 1, :] = jnp.sum(jnp.where(hit, base, 0.0), axis=0, keepdims=True)
        turn[2 + j : 3 + j, :] = gate_ref[j : j + 1, :]
    turned = turn[...].T
    slot_lane = lax.broadcasted_iota(jnp.int32, (T, S * capp), 1).astype(F32)
    picks = [jnp.where(turned[:, j : j + 1] == slot_lane, 1.0, 0.0).astype(BF16) for j in range(2)]
    for i in range(1, S):
        z_return(s, lax.rem(s + i, S)).wait_recv()
    everything = ret[...].reshape(S * capp, D)
    moe_ref[...] = (
        jnp.dot(picks[0], everything, preferred_element_type=F32) * turned[:, 2:3]
        + jnp.dot(picks[1], everything, preferred_element_type=F32) * turned[:, 3:4]
    ).astype(BF16)

    def drain(i, unused):
        to = lax.rem(s + i, S)
        z_copy(to, s).wait_send()
        z_return(to, s).wait_send()
        return unused

    lax.fori_loop(1, S, drain, jnp.int32(0))

    def drain_chunk(i, unused):
        t_reduce(i).wait_send()
        for j in range(1, X):
            x_reduce(i, other_x(j), x).wait_send()

        @pl.when((i <= s) & (s + 1 < S))
        def _():
            kv_copy(i, 1).wait_send()

        @pl.when((i >= s) & (s - 1 >= 0))
        def _():
            kv_copy(i, -1).wait_send()

        return unused

    lax.fori_loop(0, S, drain_chunk, jnp.int32(0))


def fast_kernel(
    sizes,
    q_hbm, fk_hbm, fv_hbm, sk_hbm, sv_hbm, flags_hbm, tok_hbm, ids_hbm, gate_hbm,
    up_hbm, upb_hbm, down_hbm, downb_hbm,
    attn_ref, moe_ref,
    q_v, fresh_k, fresh_v, stale_k, stale_v, flags, tok_v, ids_v, gate_v,
    up_v, upb_v, down_v, downb_v,
    disp, rows, outs, tpin, xin, fin, ret, kv, keys_v, q_in, o_out, o_in, masked, acc, stat, moe, turn,
    in_sem,
    z_send, z_recv, xf_send, xf_recv, tf_send, tf_recv,
    tr_send, tr_recv, xr_send, xr_recv, zr_send, zr_recv, kv_send, kv_recv, qo_send, qo_recv,
):
    S, X, capp = sizes
    s, x, c = lax.axis_index("seq"), lax.axis_index("exp"), lax.axis_index("tp")
    oc, ox = 1 - c, 1 - x
    T, D = tok_v.shape
    W, L = q_v.shape
    heads = W // HD
    blocks = flags.shape[0]
    blk = L // blocks

    barrier = pltpu.get_barrier_semaphore()
    for i in range(1, S):
        pl.semaphore_signal(barrier, inc=1, device_id={"seq": lax.rem(s + i, S)}, device_id_type=MESH)
    pl.semaphore_signal(barrier, inc=1, device_id={"exp": ox}, device_id_type=MESH)
    pl.semaphore_signal(barrier, inc=1, device_id={"tp": oc}, device_id_type=MESH)

    pairs = (
        (ids_hbm, ids_v), (tok_hbm, tok_v), (flags_hbm, flags),
        (fk_hbm, fresh_k), (sk_hbm, stale_k), (fv_hbm, fresh_v), (sv_hbm, stale_v),
        (up_hbm.at[0], up_v), (upb_hbm, upb_v), (down_hbm.at[0], down_v), (downb_hbm, downb_v),
        (q_hbm, q_v), (gate_hbm, gate_v),
    )
    loads = [pltpu.make_async_copy(a, b, in_sem.at[i]) for i, (a, b) in enumerate(pairs)]
    for load in loads:
        load.start()

    def rdma(src, dst, ssem, rsem, where):
        return pltpu.make_async_remote_copy(
            src_ref=src, dst_ref=dst, send_sem=ssem, recv_sem=rsem,
            device_id=where, device_id_type=MESH,
        )

    def z_copy(e, slot):
        return rdma(disp.at[e], rows.at[slot, x, c], z_send.at[e], z_recv.at[slot], {"seq": e})

    def x_forward(src, origin):
        return rdma(
            rows.at[src, origin, c], rows.at[src, origin, c],
            xf_send.at[src], xf_recv.at[src], {"exp": ox},
        )

    def t_forward(src, origin, side):
        return rdma(
            rows.at[src, origin, side], rows.at[src, origin, side],
            tf_send.at[src, origin], tf_recv.at[src, origin], {"tp": oc},
        )

    def t_reduce(src, origin):
        return rdma(
            outs.at[src, origin, oc], tpin.at[src, origin],
            tr_send.at[src, origin], tr_recv.at[src, origin], {"tp": oc},
        )

    def x_reduce(src):
        return rdma(outs.at[src, ox, c], xin.at[src], xr_send.at[src], xr_recv.at[src], {"exp": ox})

    def z_return(src, slot):
        return rdma(fin.at[src], ret.at[slot], zr_send.at[src], zr_recv.at[slot], {"seq": src})

    mate, facing = s + 1 - 2 * lax.rem(s, 2), S - 1 - s
    far = S - 1 - mate
    inner = (s != 0) & (s != S - 1)

    def kv_copy(b, part, to):
        return rdma(kv.at[b, part], kv.at[b, part], kv_send.at[b, part], kv_recv.at[b, part], {"seq": to})

    def q_copy():
        return rdma(q_v, q_in, qo_send.at[0], qo_recv.at[0], {"seq": mate})

    def o_copy():
        return rdma(o_out, o_in, qo_send.at[1], qo_recv.at[1], {"seq": mate})

    def mirrored(end, inner):
        near = jnp.where((s == 0) | (s == S - 1), end, inner)
        return jnp.where(2 * s < S, near, S - 1 - near)

    targets = [mirrored(a, b) for a, b in ((1, 2), (S - 1, 0), (2, S - 1))]
    order = [s, mate, facing, far]

    loads[0].wait()
    loads[1].wait()
    expert = lax.broadcasted_iota(jnp.int32, (S, T), 0)
    named = (ids_v[0:1, :] == expert) | (ids_v[1:2, :] == expert)
    earlier = lax.broadcasted_iota(jnp.int32, (T, T), 0) < lax.broadcasted_iota(jnp.int32, (T, T), 1)
    place = jnp.dot(
        jnp.where(named, 1.0, 0.0).astype(BF16),
        jnp.where(earlier, 1.0, 0.0).astype(BF16),
        preferred_element_type=F32,
    )
    slotted = jnp.where(named, place, -1.0)
    slot_rows = lax.broadcasted_iota(jnp.int32, (capp, T), 0).astype(F32)
    for e in range(S):
        pick = jnp.where(slotted[e : e + 1, :] == slot_rows, 1.0, 0.0).astype(BF16)
        disp[e] = jnp.dot(pick, tok_v[...], preferred_element_type=F32).astype(BF16)
    rows[s, x, c] = disp[s]
    for load in loads[2:7]:
        load.wait()
    for b in range(blocks):
        fresh = flags[b] == 1
        part = pl.ds(b * blk, blk)
        kv[s, 0, :, part] = jnp.where(fresh, fresh_k[:, part], stale_k[:, part])
        kv[s, 1, :, part] = jnp.where(fresh, fresh_v[:, part], stale_v[:, part])

    pl.semaphore_wait(barrier, S - 1 + 1 + 1)

    def forward(src):
        x_forward(src, x).start()
        t_forward(src, x, c).start()

    def arrive(src):
        z_copy(src, src).wait_recv()
        forward(src)

    for e in targets:
        z_copy(e, s).start()
    forward(s)

    onward = jnp.where(inner, facing, mate)
    kv_copy(s, 0, onward).start()
    kv_copy(s, 1, onward).start()

    for load in loads[7:]:
        load.wait()

    @pl.when(jnp.logical_not(inner))
    def _():
        q_copy().start()

    scale = 1.0 / math.sqrt(HD)
    channel = lax.broadcasted_iota(jnp.int32, (W, L), 0)

    def ask(i, source):
        for h in range(heads):
            own = (channel >= h * HD) & (channel < (h + 1) * HD)
            masked[i, h] = jnp.where(own, source[...].astype(F32), 0.0).astype(BF16)

    def take(b):
        keys_v[b] = kv[b, 0].T

    def attend(i, b, first=False):
        for h in range(heads):
            lo, hi = h * HD, (h + 1) * HD
            a, z = lo // 128 * 128, min(-(-hi // 128) * 128, W)
            scores = jnp.dot(keys_v[b, :, a:z], masked[i, h, a:z, :], preferred_element_type=F32) * scale
            top = jnp.max(scores, axis=0, keepdims=True)
            if not first:
                before = stat[i, h : h + 1, :]
                top = jnp.maximum(before, top)
                fade = jnp.exp(before - top)
            probs = jnp.exp(scores - top)
            total = jnp.sum(probs, axis=0, keepdims=True)
            a, z = lo // 16 * 16, -(-hi // 16) * 16
            mixed = jnp.dot(kv[b, 1, a:z, :], probs.astype(BF16), preferred_element_type=F32)
            mixed = mixed[lo - a : hi - a]
            if not first:
                total = stat[i, heads + h : heads + h + 1, :] * fade + total
                mixed = acc[i, lo:hi, :] * fade + mixed
            stat[i, h : h + 1, :] = top
            stat[i, heads + h : heads + h + 1, :] = total
            acc[i, lo:hi, :] = mixed

    def answer(i):
        for h in range(heads):
            lo, hi = h * HD, (h + 1) * HD
            acc[i, lo:hi, :] = acc[i, lo:hi, :] / stat[i, heads + h : heads + h + 1, :]
        return acc[i].astype(BF16)

    def mlp(src, origin):
        block = rows[src, origin].reshape(2 * capp, D)
        hidden = jnp.dot(block, up_v[...], preferred_element_type=F32) + upb_v[...]
        hidden = jax.nn.gelu(hidden).astype(BF16)
        result = jnp.dot(hidden, down_v[...], preferred_element_type=F32).astype(BF16)
        outs[src, origin] = result.reshape(2, capp, D)
        t_reduce(src, origin).start()

    def mine(src):
        t_forward(src, x, oc).wait_recv()
        mlp(src, x)

    def crossed(src):
        x_forward(src, ox).wait_recv()
        t_forward(src, ox, c).start()

    def other(src):
        t_forward(src, ox, oc).wait_recv()
        mlp(src, ox)

    def reduce(src):
        t_reduce(src, ox).wait_recv()
        outs[src, ox, c] = (outs[src, ox, c].astype(F32) + tpin[src, ox].astype(F32)).astype(BF16)
        x_reduce(src).start()

    def finish(src):
        t_reduce(src, x).wait_recv()
        total = outs[src, x, c].astype(F32) + tpin[src, x].astype(F32) + downb_v[...]
        x_reduce(src).wait_recv()
        return (total + xin[src].astype(F32)).astype(BF16)

    def finish_send(src):
        fin[src] = finish(src)
        z_return(src, s).start()

    o0, o1, o2, o3 = order
    mine(o0)
    turn[...] = jnp.zeros_like(turn)
    for i, e in enumerate(order):
        hit = [ids_v[j : j + 1, :] == e for j in range(2)]
        spot = jnp.sum(jnp.where(expert == e, place, 0.0), axis=0, keepdims=True)
        turn[i : i + 1, :] = jnp.where(hit[0] | hit[1], spot, -1.0)
        turn[S + i : S + i + 1, :] = sum(
            jnp.where(hit[j], gate_v[j : j + 1, :], 0.0) for j in range(2)
        )
    turned = turn[...].T
    slot_lane = lax.broadcasted_iota(jnp.int32, (T, capp), 1).astype(F32)

    outer = jnp.logical_not(inner)
    r1, r2, r3 = (jnp.where(inner, a, b) for a, b in ((o1, o2), (o2, o3), (o3, o1)))

    @pl.when(inner)
    def _():
        ask(0, q_v)
        take(s)
        attend(0, s, first=True)

    arrive(o1)

    @pl.when(inner)
    def _():
        arrive(o2)

    crossed(o0)
    mine(o1)
    other(o0)
    crossed(o1)

    @pl.when(outer)
    def _():
        arrive(o2)

    other(o1)
    mine(o2)

    @pl.when(outer)
    def _():
        arrive(o3)

    crossed(o2)

    @pl.when(inner)
    def _():
        arrive(o3)
        reduce(o1)
        kv_copy(mate, 0, mate).wait_recv()
        kv_copy(mate, 0, facing).start()

    other(o2)
    mine(o3)
    reduce(o2)

    @pl.when(inner)
    def _():
        kv_copy(mate, 1, mate).wait_recv()
        kv_copy(mate, 1, facing).start()
        take(mate)

    crossed(o3)

    @pl.when(inner)
    def _():
        attend(0, mate)

    other(o3)

    @pl.when(inner)
    def _():
        q_copy().wait_recv()
        ask(1, q_in)
        attend(1, s, first=True)

    reduce(o3)

    @pl.when(outer)
    def _():
        reduce(o1)

    reduce(o0)
    finish_send(r1)

    @pl.when(inner)
    def _():
        attend(1, mate)
        kv_copy(facing, 0, facing).wait_recv()
        kv_copy(facing, 1, facing).wait_recv()
        take(facing)
        attend(1, facing)
        attend(0, facing)

    finish_send(r2)

    @pl.when(inner)
    def _():
        kv_copy(far, 0, facing).wait_recv()
        kv_copy(far, 1, facing).wait_recv()
        take(far)
        attend(1, far)
        o_out[...] = answer(1)
        o_copy().start()
        attend(0, far)
        attn_ref[...] = answer(0)

    finish_send(r3)

    def combine(i, values):
        pick = jnp.where(turned[:, i : i + 1] == slot_lane, 1.0, 0.0).astype(BF16)
        return jnp.dot(pick, values, preferred_element_type=F32) * turned[:, S + i : S + i + 1]

    moe[...] = combine(0, finish(s))
    for i in range(1, S - 1):
        z_return(s, order[i]).wait_recv()
        moe[...] += combine(i, ret[order[i]])

    @pl.when(jnp.logical_not(inner))
    def _():
        o_copy().wait_recv()
        attn_ref[...] = o_in[...]

    z_return(s, order[S - 1]).wait_recv()
    moe_ref[...] = (moe[...] + combine(S - 1, ret[order[S - 1]])).astype(BF16)

    def drain(i, unused):
        to = lax.rem(s + i, S)
        z_copy(to, s).wait_send()
        z_return(to, s).wait_send()
        return unused

    lax.fori_loop(1, S, drain, jnp.int32(0))

    def drain_chunk(i, unused):
        x_forward(i, x).wait_send()
        x_reduce(i).wait_send()
        for origin in range(X):
            t_forward(i, origin, c).wait_send()
            t_reduce(i, origin).wait_send()
        return unused

    lax.fori_loop(0, S, drain_chunk, jnp.int32(0))
    for part in range(2):
        kv_copy(s, part, onward).wait_send()

    @pl.when(inner)
    def _():
        for part in range(2):
            kv_copy(mate, part, facing).wait_send()
        o_copy().wait_send()

    @pl.when(jnp.logical_not(inner))
    def _():
        q_copy().wait_send()


def fast_call(S, X, capp, args):
    q, tok, up, flags = args[0], args[6], args[9], args[5]
    width, length = q.shape
    tokens, D = tok.shape
    hidden = up.shape[2]
    hbm = pl.BlockSpec(memory_space=pltpu.HBM)
    vmem = pl.BlockSpec(memory_space=pltpu.VMEM)
    dma = pltpu.SemaphoreType.DMA
    half = pltpu.VMEM((width, length), BF16)
    slots = pltpu.VMEM((S, capp, D), BF16)
    return pl.pallas_call(
        functools.partial(fast_kernel, (S, X, capp)),
        out_shape=(
            jax.ShapeDtypeStruct((width, length), BF16),
            jax.ShapeDtypeStruct((tokens, D), BF16),
        ),
        in_specs=[hbm] * 13,
        out_specs=(vmem, vmem),
        scratch_shapes=[
            half, half, half, half, half,
            pltpu.SMEM(flags.shape, jnp.int32),
            pltpu.VMEM((tokens, D), BF16),
            pltpu.VMEM((2, tokens), jnp.int32),
            pltpu.VMEM((2, tokens), F32),
            pltpu.VMEM((D, hidden), BF16),
            pltpu.VMEM((1, hidden), F32),
            pltpu.VMEM((hidden, D), BF16),
            pltpu.VMEM((1, D), F32),
            slots,
            pltpu.VMEM((S, X, 2, capp, D), BF16),
            pltpu.VMEM((S, X, 2, capp, D), BF16),
            pltpu.VMEM((S, X, capp, D), BF16),
            slots, slots, slots,
            pltpu.VMEM((S, 2, width, length), BF16),
            pltpu.VMEM((S, length, width), BF16),
            half, half, half,
            pltpu.VMEM((2, width // HD, width, length), BF16),
            pltpu.VMEM((2, width, length), F32),
            pltpu.VMEM((2, 2 * width // HD, length), F32),
            pltpu.VMEM((tokens, D), F32),
            pltpu.VMEM((128, tokens), F32),
            dma((13,)),
            dma((S,)), dma((S,)), dma((S,)), dma((S,)), dma((S, X)), dma((S, X)),
            dma((S, X)), dma((S, X)), dma((S,)), dma((S,)), dma((S,)), dma((S,)),
            dma((S, 2)), dma((S, 2)), dma((2,)), dma((2,)),
        ],
        compiler_params=pltpu.CompilerParams(
            collective_id=0, has_side_effects=True, vmem_limit_bytes=VMEM_LIMIT
        ),
    )(*[pltpu.with_memory_space_constraint(a, pltpu.HBM) for a in args])


def local(
    attn_query, fresh_keys, fresh_values, stale_keys, stale_values, block_flags,
    moe_tokens, expert_ids, gate_weights, up_weight, up_bias, down_weight, down_bias,
):
    S, X = lax.axis_size("seq"), lax.axis_size("exp")
    assert lax.axis_size("tp") == 2 and up_weight.shape[0] == 1
    tokens, D = moe_tokens.shape
    length, width = attn_query.shape
    hidden = up_weight.shape[2]
    cap = 5 * tokens // (2 * S)
    capp = -(-cap // 16) * 16
    if (S, X) == (4, 2):
        attn_out, moe_out = fast_call(S, X, capp, (
            attn_query.T, fresh_keys.T, fresh_values.T, stale_keys.T, stale_values.T, block_flags,
            moe_tokens, expert_ids.T, gate_weights.T,
            up_weight, up_bias, down_weight, down_bias,
        ))
        return attn_out.T, moe_out
    vmem = pl.BlockSpec(memory_space=pltpu.VMEM)
    smem = pl.BlockSpec(memory_space=pltpu.SMEM)
    hbm = pl.BlockSpec(memory_space=pl.ANY)
    dma = pltpu.SemaphoreType.DMA
    attn_out, moe_out = pl.pallas_call(
        functools.partial(layer_kernel, (S, X, capp)),
        out_shape=(
            jax.ShapeDtypeStruct((width, length), BF16),
            jax.ShapeDtypeStruct((tokens, D), BF16),
        ),
        in_specs=[vmem] * 5 + [smem] + [vmem] * 3 + [hbm, vmem, hbm, vmem],
        out_specs=(vmem, vmem),
        scratch_shapes=[
            pltpu.VMEM((D, hidden), BF16),
            pltpu.VMEM((hidden, D), BF16),
            pltpu.VMEM((S, tokens), F32),
            pltpu.VMEM((S, capp, D), BF16),
            pltpu.VMEM((S, 2, X, capp, D), BF16),
            pltpu.VMEM((S, X, capp, D), BF16),
            pltpu.VMEM((S, X, capp, D), BF16),
            pltpu.VMEM((S, capp, D), BF16),
            pltpu.VMEM((S, capp, D), BF16),
            pltpu.VMEM((S, 2, width, length), BF16),
            pltpu.VMEM((S * length, width), BF16),
            pltpu.VMEM((width, length), F32),
            pltpu.VMEM((128, tokens), F32),
            dma((2,)),
            dma((S,)), dma((S,)), dma((S, X)), dma((S, X)), dma((S, X)), dma((S, X)),
            dma((S,)), dma((S,)), dma((S, X)), dma((S, X)), dma((S,)), dma((S,)),
            dma((S,)), dma((S,)), dma((S,)),
        ],
        compiler_params=pltpu.CompilerParams(
            collective_id=0, has_side_effects=True, vmem_limit_bytes=67043328
        ),
    )(
        attn_query.T, fresh_keys.T, fresh_values.T, stale_keys.T, stale_values.T, block_flags,
        moe_tokens, expert_ids.T, gate_weights.T,
        up_weight, up_bias, down_weight, down_bias,
    )
    return attn_out.T, moe_out


def solution(mesh):
    in_specs = (
        P(("groups", "seq"), ("exp", "tp")),
        P(("groups", "seq"), ("exp", "tp")),
        P(("groups", "seq"), ("exp", "tp")),
        P(("groups", "seq"), ("exp", "tp")),
        P(("groups", "seq"), ("exp", "tp")),
        P(("groups", "seq")),
        P(("groups", "seq", "exp", "tp"), None),
        P(("groups", "seq", "exp", "tp"), None),
        P(("groups", "seq", "exp", "tp"), None),
        P("seq", None, ("exp", "tp")),
        P("seq", ("exp", "tp")),
        P("seq", ("exp", "tp"), None),
        P("seq", None),
    )
    out_specs = (P(("groups", "seq"), ("exp", "tp")), P(("groups", "seq", "exp", "tp"), None))
    return jax.shard_map(local, mesh=mesh, in_specs=in_specs, out_specs=out_specs, check_vma=False)
```

```python
import functools
import math

import jax
import jax.numpy as jnp
from jax import lax
from jax.experimental import pallas as pl
from jax.experimental.pallas import tpu as pltpu
from jax.sharding import PartitionSpec as P

HD = 72
MESH = pl.DeviceIdType.MESH
F32 = jnp.float32
BF16 = jnp.bfloat16
VMEM_LIMIT = 40 * 1024 * 1024


def layer_kernel(
    sizes,
    q_ref, fresh_k, fresh_v, stale_k, stale_v, flags,
    tok_ref, ids_ref, gate_ref,
    up_hbm, upb_ref, down_hbm, downb_ref,
    attn_ref, moe_ref,
    up_v, down_v, place_v, disp, rows, tpin, xin, fin, ret, kv, keys_v, acc, turn,
    w_sem,
    z_send, z_recv, xf_send, xf_recv, tf_send, tf_recv,
    tr_send, tr_recv, xr_send, xr_recv, zr_send, zr_recv, kv_right, kv_left, kv_recv,
):
    S, X, capp = sizes
    s, x, c = lax.axis_index("seq"), lax.axis_index("exp"), lax.axis_index("tp")
    oc = 1 - c
    T, D = tok_ref.shape
    W, L = q_ref.shape
    heads = W // HD
    blk = L // flags.shape[0]

    up_copy = pltpu.make_async_copy(up_hbm.at[0], up_v, w_sem.at[0])
    down_copy = pltpu.make_async_copy(down_hbm.at[0], down_v, w_sem.at[1])
    up_copy.start()
    down_copy.start()

    def rdma(src, dst, ssem, rsem, where):
        return pltpu.make_async_remote_copy(
            src_ref=src, dst_ref=dst, send_sem=ssem, recv_sem=rsem,
            device_id=where, device_id_type=MESH,
        )

    def z_copy(e, slot):
        return rdma(disp.at[e], rows.at[slot, c, x], z_send.at[e], z_recv.at[slot], {"seq": e})

    def x_forward(src, to, origin):
        return rdma(
            rows.at[src, c, origin], rows.at[src, c, origin],
            xf_send.at[src, to], xf_recv.at[src, origin], {"exp": to},
        )

    def t_forward(src, origin, side):
        return rdma(
            rows.at[src, side, origin], rows.at[src, side, origin],
            tf_send.at[src, origin], tf_recv.at[src, origin], {"tp": oc},
        )

    def t_reduce(src):
        return rdma(rows.at[src, oc], tpin.at[src], tr_send.at[src], tr_recv.at[src], {"tp": oc})

    def x_reduce(src, to, origin):
        return rdma(
            rows.at[src, c, to], xin.at[src, origin],
            xr_send.at[src, to], xr_recv.at[src, origin], {"exp": to},
        )

    def z_return(src, slot):
        return rdma(fin.at[src], ret.at[slot], zr_send.at[src], zr_recv.at[slot], {"seq": src})

    def kv_copy(b, step):
        sems = kv_right if step > 0 else kv_left
        return rdma(kv.at[b], kv.at[b], sems.at[b], kv_recv.at[b], {"seq": s + step})

    def other_x(i):
        return lax.rem(x + i, X)

    def order(k):
        side = jnp.minimum(s, S - 1 - s)
        near = k // 2 + 1
        near = jnp.where(lax.rem(k, 2) == 0, near, -near)
        far = k - side + 1
        far = jnp.where(2 * s < S, far, -far)
        step = jnp.where(k < 2 * side, near, far)
        return s + jnp.where(k == S - 1, 0, step)

    barrier = pltpu.get_barrier_semaphore()
    for i in range(1, S):
        pl.semaphore_signal(barrier, inc=1, device_id={"seq": lax.rem(s + i, S)}, device_id_type=MESH)
    for i in range(1, X):
        pl.semaphore_signal(barrier, inc=1, device_id={"exp": other_x(i)}, device_id_type=MESH)
    pl.semaphore_signal(barrier, inc=1, device_id={"tp": oc}, device_id_type=MESH)

    expert = lax.broadcasted_iota(jnp.int32, (S, T), 0)
    named = (ids_ref[0:1, :] == expert) | (ids_ref[1:2, :] == expert)
    earlier = lax.broadcasted_iota(jnp.int32, (T, T), 0) < lax.broadcasted_iota(jnp.int32, (T, T), 1)
    place = jnp.dot(
        jnp.where(named, 1.0, 0.0).astype(BF16),
        jnp.where(earlier, 1.0, 0.0).astype(BF16),
        preferred_element_type=F32,
    )
    place_v[...] = jnp.where(named, place, -1.0)
    slot_rows = lax.broadcasted_iota(jnp.int32, (capp, T), 0).astype(F32)

    def slots_of(e):
        pick = jnp.where(place_v[pl.ds(e, 1), :] == slot_rows, 1.0, 0.0).astype(BF16)
        return jnp.dot(pick, tok_ref[...], preferred_element_type=F32).astype(BF16)

    def forward(src):
        for i in range(1, X):
            x_forward(src, other_x(i), x).start()
        t_forward(src, x, c).start()

    rows[s, c, x] = slots_of(s)
    pl.semaphore_wait(barrier, S - 1 + X - 1 + 1)
    forward(s)
    def dispatch(k):
        e = order(jnp.int32(k))
        disp[e] = slots_of(e)
        z_copy(e, s).start()

    for k in range(min(2, S - 1)):
        dispatch(k)
    for b in range(flags.shape[0]):
        fresh = flags[b] == 1
        part = pl.ds(b * blk, blk)
        kv[s, 0, :, part] = jnp.where(fresh, fresh_k[:, part], stale_k[:, part])
        kv[s, 1, :, part] = jnp.where(fresh, fresh_v[:, part], stale_v[:, part])

    def relay(step):
        low, high = s - (step - 1), s + (step - 1)

        @pl.when(low >= 0)
        def _():
            @pl.when(low < s)
            def _():
                kv_copy(low, 1).wait_recv()

            @pl.when(s + 1 < S)
            def _():
                kv_copy(low, 1).start()

        @pl.when(high < S)
        def _():
            @pl.when(high > s)
            def _():
                kv_copy(high, -1).wait_recv()

            @pl.when(s - 1 >= 0)
            def _():
                kv_copy(high, -1).start()

    relay(1)
    for k in range(2, S - 1):
        dispatch(k)
    nearest = order(jnp.int32(0))
    z_copy(nearest, nearest).wait_recv()
    forward(nearest)

    up_copy.wait()
    down_copy.wait()

    def finish(src):
        total = rows[src, c, x].astype(F32) + downb_ref[...]
        for i in range(1, X):
            x_reduce(src, other_x(i), other_x(i)).wait_recv()
            total = total + xin[src, other_x(i)].astype(F32)
        done = total.astype(BF16)
        fin[src] = done

    def finish_send(src):
        finish(src)

        @pl.when(src != s)
        def _():
            z_return(src, s).start()

        @pl.when(src == s)
        def _():
            ret[s] = fin[s]

    def chunk(k, unused):
        src = order(k)
        for i in range(1, X):
            x_forward(src, other_x(i), other_x(i)).wait_recv()
            t_forward(src, other_x(i), c).start()

        @pl.when(k + 1 < S - 1)
        def _():
            nxt = order(k + 1)
            z_copy(nxt, nxt).wait_recv()
            forward(nxt)

        for i in range(X):
            t_forward(src, other_x(i), oc).wait_recv()
        for i in range(1, X):
            x_forward(src, other_x(i), x).wait_send()
        for i in range(X):
            t_forward(src, other_x(i), c).wait_send()

        block = rows[src].reshape(2 * X * capp, D)
        hidden = jnp.dot(block, up_v[...], preferred_element_type=F32) + upb_ref[...]
        hidden = jax.nn.gelu(hidden).astype(BF16)
        result = jnp.dot(hidden, down_v[...], preferred_element_type=F32).astype(BF16)
        rows[src] = result.reshape(2, X, capp, D)
        t_reduce(src).start()

        @pl.when(k >= 1)
        def _():
            finish_send(order(k - 1))

        @pl.when(k == 0)
        def _():
            relay(2)

        @pl.when((k >= 2) & (k < S - 1))
        def _():
            relay(k + 1)

        t_reduce(src).wait_recv()
        for i in range(X):
            to = other_x(i)
            rows[src, c, to] = (rows[src, c, to].astype(F32) + tpin[src, to].astype(F32)).astype(BF16)
            if i > 0:
                x_reduce(src, to, x).start()
        return unused

    lax.fori_loop(0, S, chunk, jnp.int32(0))

    relay(S)

    for i in range(S):
        keys_v[pl.ds(i * L, L), :] = kv[i, 0].T
    scale = 1.0 / math.sqrt(HD)
    channel = lax.broadcasted_iota(jnp.int32, (W, L), 0)

    def head(h, unused):
        mine = (channel >= h * HD) & (channel < (h + 1) * HD)
        query = jnp.where(mine, q_ref[...].astype(F32), 0.0).astype(BF16)
        scores = jnp.dot(keys_v[...], query, preferred_element_type=F32) * scale
        probs = jnp.exp(scores - jnp.max(scores, axis=0, keepdims=True))
        total = jnp.sum(probs, axis=0, keepdims=True)
        weights = probs.astype(BF16)
        mixed = jnp.zeros((W, L), F32)
        for i in range(S):
            mixed += jnp.dot(kv[i, 1], weights[i * L : (i + 1) * L], preferred_element_type=F32)
        acc[...] = jnp.where(mine, mixed / total, acc[...])
        return unused

    acc[...] = jnp.zeros_like(acc)
    lax.fori_loop(0, heads, head, jnp.int32(0))
    attn_ref[...] = acc[...].astype(BF16)
    finish_send(s)

    base = jnp.where(named, place, 0.0) + (expert * capp).astype(F32)
    turn[...] = jnp.zeros_like(turn)
    for j in range(2):
        hit = ids_ref[j : j + 1, :] == expert
        turn[j : j + 1, :] = jnp.sum(jnp.where(hit, base, 0.0), axis=0, keepdims=True)
        turn[2 + j : 3 + j, :] = gate_ref[j : j + 1, :]
    turned = turn[...].T
    slot_lane = lax.broadcasted_iota(jnp.int32, (T, S * capp), 1).astype(F32)
    picks = [jnp.where(turned[:, j : j + 1] == slot_lane, 1.0, 0.0).astype(BF16) for j in range(2)]
    for i in range(1, S):
        z_return(s, lax.rem(s + i, S)).wait_recv()
    everything = ret[...].reshape(S * capp, D)
    moe_ref[...] = (
        jnp.dot(picks[0], everything, preferred_element_type=F32) * turned[:, 2:3]
        + jnp.dot(picks[1], everything, preferred_element_type=F32) * turned[:, 3:4]
    ).astype(BF16)

    def drain(i, unused):
        to = lax.rem(s + i, S)
        z_copy(to, s).wait_send()
        z_return(to, s).wait_send()
        return unused

    lax.fori_loop(1, S, drain, jnp.int32(0))

    def drain_chunk(i, unused):
        t_reduce(i).wait_send()
        for j in range(1, X):
            x_reduce(i, other_x(j), x).wait_send()

        @pl.when((i <= s) & (s + 1 < S))
        def _():
            kv_copy(i, 1).wait_send()

        @pl.when((i >= s) & (s - 1 >= 0))
        def _():
            kv_copy(i, -1).wait_send()

        return unused

    lax.fori_loop(0, S, drain_chunk, jnp.int32(0))


def fast_kernel(
    sizes,
    q_hbm, fk_hbm, fv_hbm, sk_hbm, sv_hbm, flags_hbm, tok_hbm, ids_hbm, gate_hbm,
    up_hbm, upb_hbm, down_hbm, downb_hbm,
    attn_ref, moe_ref,
    q_v, fresh_k, fresh_v, stale_k, stale_v, flags, tok_v, ids_v, gate_v,
    up_v, upb_v, down_v, downb_v,
    disp, rows, outs, tpin, xin, fin, ret, kv, keys_v, q_in, o_out, o_in, masked, acc, stat, moe, turn,
    in_sem,
    z_send, z_recv, xf_send, xf_recv, tf_send, tf_recv,
    tr_send, tr_recv, xr_send, xr_recv, zr_send, zr_recv, kv_send, kv_recv, qo_send, qo_recv,
):
    S, X, capp = sizes
    s, x, c = lax.axis_index("seq"), lax.axis_index("exp"), lax.axis_index("tp")
    oc, ox = 1 - c, 1 - x
    T, D = tok_v.shape
    W, L = q_v.shape
    heads = W // HD
    blocks = flags.shape[0]
    blk = L // blocks

    barrier = pltpu.get_barrier_semaphore()
    for i in range(1, S):
        pl.semaphore_signal(barrier, inc=1, device_id={"seq": lax.rem(s + i, S)}, device_id_type=MESH)
    pl.semaphore_signal(barrier, inc=1, device_id={"exp": ox}, device_id_type=MESH)
    pl.semaphore_signal(barrier, inc=1, device_id={"tp": oc}, device_id_type=MESH)

    pairs = (
        (ids_hbm, ids_v), (tok_hbm, tok_v), (flags_hbm, flags),
        (fk_hbm, fresh_k), (sk_hbm, stale_k), (fv_hbm, fresh_v), (sv_hbm, stale_v),
        (up_hbm.at[0], up_v), (upb_hbm, upb_v), (down_hbm.at[0], down_v), (downb_hbm, downb_v),
        (q_hbm, q_v), (gate_hbm, gate_v),
    )
    loads = [pltpu.make_async_copy(a, b, in_sem.at[i]) for i, (a, b) in enumerate(pairs)]
    for load in loads:
        load.start()

    def rdma(src, dst, ssem, rsem, where):
        return pltpu.make_async_remote_copy(
            src_ref=src, dst_ref=dst, send_sem=ssem, recv_sem=rsem,
            device_id=where, device_id_type=MESH,
        )

    def z_copy(e, slot):
        return rdma(disp.at[e], rows.at[slot, x, c], z_send.at[e], z_recv.at[slot], {"seq": e})

    def x_forward(src, origin):
        return rdma(
            rows.at[src, origin, c], rows.at[src, origin, c],
            xf_send.at[src], xf_recv.at[src], {"exp": ox},
        )

    def t_forward(src, origin, side):
        return rdma(
            rows.at[src, origin, side], rows.at[src, origin, side],
            tf_send.at[src, origin], tf_recv.at[src, origin], {"tp": oc},
        )

    def t_reduce(src, origin):
        return rdma(
            outs.at[src, origin, oc], tpin.at[src, origin],
            tr_send.at[src, origin], tr_recv.at[src, origin], {"tp": oc},
        )

    def x_reduce(src):
        return rdma(outs.at[src, ox, c], xin.at[src], xr_send.at[src], xr_recv.at[src], {"exp": ox})

    def z_return(src, slot):
        return rdma(fin.at[src], ret.at[slot], zr_send.at[src], zr_recv.at[slot], {"seq": src})

    mate, facing = s + 1 - 2 * lax.rem(s, 2), S - 1 - s
    far = S - 1 - mate
    inner = (s != 0) & (s != S - 1)

    def kv_copy(b, part, to):
        return rdma(kv.at[b, part], kv.at[b, part], kv_send.at[b, part], kv_recv.at[b, part], {"seq": to})

    def q_copy():
        return rdma(q_v, q_in, qo_send.at[0], qo_recv.at[0], {"seq": mate})

    def o_copy():
        return rdma(o_out, o_in, qo_send.at[1], qo_recv.at[1], {"seq": mate})

    def mirrored(end, inner):
        near = jnp.where((s == 0) | (s == S - 1), end, inner)
        return jnp.where(2 * s < S, near, S - 1 - near)

    targets = [mirrored(a, b) for a, b in ((1, 2), (S - 1, 0), (2, S - 1))]
    order = [s, mate, facing, far]

    loads[0].wait()
    loads[1].wait()
    expert = lax.broadcasted_iota(jnp.int32, (S, T), 0)
    named = (ids_v[0:1, :] == expert) | (ids_v[1:2, :] == expert)
    earlier = lax.broadcasted_iota(jnp.int32, (T, T), 0) < lax.broadcasted_iota(jnp.int32, (T, T), 1)
    place = jnp.dot(
        jnp.where(named, 1.0, 0.0).astype(BF16),
        jnp.where(earlier, 1.0, 0.0).astype(BF16),
        preferred_element_type=F32,
    )
    slotted = jnp.where(named, place, -1.0)
    slot_rows = lax.broadcasted_iota(jnp.int32, (capp, T), 0).astype(F32)
    for e in range(S):
        pick = jnp.where(slotted[e : e + 1, :] == slot_rows, 1.0, 0.0).astype(BF16)
        disp[e] = jnp.dot(pick, tok_v[...], preferred_element_type=F32).astype(BF16)
    rows[s, x, c] = disp[s]
    for load in loads[2:7]:
        load.wait()
    for b in range(blocks):
        fresh = flags[b] == 1
        part = pl.ds(b * blk, blk)
        kv[s, 0, :, part] = jnp.where(fresh, fresh_k[:, part], stale_k[:, part])
        kv[s, 1, :, part] = jnp.where(fresh, fresh_v[:, part], stale_v[:, part])

    pl.semaphore_wait(barrier, S - 1 + 1 + 1)

    def forward(src):
        x_forward(src, x).start()
        t_forward(src, x, c).start()

    def arrive(src):
        z_copy(src, src).wait_recv()
        forward(src)

    for e in targets:
        z_copy(e, s).start()
    forward(s)

    onward = jnp.where(inner, facing, mate)
    kv_copy(s, 0, onward).start()
    kv_copy(s, 1, onward).start()

    for load in loads[7:]:
        load.wait()

    @pl.when(jnp.logical_not(inner))
    def _():
        q_copy().start()

    scale = 1.0 / math.sqrt(HD)
    channel = lax.broadcasted_iota(jnp.int32, (W, L), 0)

    def ask(i, source):
        for h in range(heads):
            own = (channel >= h * HD) & (channel < (h + 1) * HD)
            masked[i, h] = jnp.where(own, source[...].astype(F32), 0.0).astype(BF16)

    def take(b):
        keys_v[b] = kv[b, 0].T

    def attend(i, b, first=False):
        for h in range(heads):
            lo, hi = h * HD, (h + 1) * HD
            a, z = lo // 128 * 128, min(-(-hi // 128) * 128, W)
            scores = jnp.dot(keys_v[b, :, a:z], masked[i, h, a:z, :], preferred_element_type=F32) * scale
            top = jnp.max(scores, axis=0, keepdims=True)
            if not first:
                before = stat[i, h : h + 1, :]
                top = jnp.maximum(before, top)
                fade = jnp.exp(before - top)
            probs = jnp.exp(scores - top)
            total = jnp.sum(probs, axis=0, keepdims=True)
            a, z = lo // 16 * 16, -(-hi // 16) * 16
            mixed = jnp.dot(kv[b, 1, a:z, :], probs.astype(BF16), preferred_element_type=F32)
            mixed = mixed[lo - a : hi - a]
            if not first:
                total = stat[i, heads + h : heads + h + 1, :] * fade + total
                mixed = acc[i, lo:hi, :] * fade + mixed
            stat[i, h : h + 1, :] = top
            stat[i, heads + h : heads + h + 1, :] = total
            acc[i, lo:hi, :] = mixed

    def answer(i):
        for h in range(heads):
            lo, hi = h * HD, (h + 1) * HD
            acc[i, lo:hi, :] = acc[i, lo:hi, :] / stat[i, heads + h : heads + h + 1, :]
        return acc[i].astype(BF16)

    def mlp(src, origin):
        block = rows[src, origin].reshape(2 * capp, D)
        hidden = jnp.dot(block, up_v[...], preferred_element_type=F32) + upb_v[...]
        hidden = jax.nn.gelu(hidden).astype(BF16)
        result = jnp.dot(hidden, down_v[...], preferred_element_type=F32).astype(BF16)
        outs[src, origin] = result.reshape(2, capp, D)
        t_reduce(src, origin).start()

    def mine(src):
        t_forward(src, x, oc).wait_recv()
        mlp(src, x)

    def crossed(src):
        x_forward(src, ox).wait_recv()
        t_forward(src, ox, c).start()

    def other(src):
        t_forward(src, ox, oc).wait_recv()
        mlp(src, ox)

    def reduce(src):
        t_reduce(src, ox).wait_recv()
        outs[src, ox, c] = (outs[src, ox, c].astype(F32) + tpin[src, ox].astype(F32)).astype(BF16)
        x_reduce(src).start()

    def finish(src):
        t_reduce(src, x).wait_recv()
        total = outs[src, x, c].astype(F32) + tpin[src, x].astype(F32) + downb_v[...]
        x_reduce(src).wait_recv()
        return (total + xin[src].astype(F32)).astype(BF16)

    def finish_send(src):
        fin[src] = finish(src)
        z_return(src, s).start()

    o0, o1, o2, o3 = order
    mine(o0)
    turn[...] = jnp.zeros_like(turn)
    for i, e in enumerate(order):
        hit = [ids_v[j : j + 1, :] == e for j in range(2)]
        spot = jnp.sum(jnp.where(expert == e, place, 0.0), axis=0, keepdims=True)
        turn[i : i + 1, :] = jnp.where(hit[0] | hit[1], spot, -1.0)
        turn[S + i : S + i + 1, :] = sum(
            jnp.where(hit[j], gate_v[j : j + 1, :], 0.0) for j in range(2)
        )
    turned = turn[...].T
    slot_lane = lax.broadcasted_iota(jnp.int32, (T, capp), 1).astype(F32)

    outer = jnp.logical_not(inner)
    r1, r3 = jnp.where(inner, o1, o2), jnp.where(inner, o3, o1)

    @pl.when(inner)
    def _():
        ask(0, q_v)
        take(s)
        attend(0, s, first=True)

    arrive(o1)

    @pl.when(inner)
    def _():
        arrive(o2)

    crossed(o0)
    mine(o1)
    other(o0)
    crossed(o1)

    @pl.when(outer)
    def _():
        arrive(o2)

    other(o1)
    mine(o2)

    @pl.when(outer)
    def _():
        arrive(o3)

    crossed(o2)

    @pl.when(inner)
    def _():
        arrive(o3)
        reduce(o1)
        kv_copy(mate, 0, mate).wait_recv()
        kv_copy(mate, 0, facing).start()

    other(o2)
    mine(o3)
    reduce(o2)

    @pl.when(inner)
    def _():
        kv_copy(mate, 1, mate).wait_recv()
        kv_copy(mate, 1, facing).start()
        take(mate)

    crossed(o3)

    @pl.when(inner)
    def _():
        attend(0, mate)

    other(o3)

    @pl.when(inner)
    def _():
        q_copy().wait_recv()
        ask(1, q_in)
        attend(1, s, first=True)

    reduce(o3)

    @pl.when(outer)
    def _():
        reduce(o1)

    reduce(o0)
    finish_send(r1)

    @pl.when(inner)
    def _():
        attend(1, mate)
        kv_copy(facing, 0, facing).wait_recv()
        kv_copy(facing, 1, facing).wait_recv()
        take(facing)
        attend(1, facing)
        attend(0, facing)

    @pl.when(outer)
    def _():
        finish_send(o3)

    @pl.when(inner)
    def _():
        kv_copy(far, 0, facing).wait_recv()
        kv_copy(far, 1, facing).wait_recv()
        take(far)
        attend(1, far)
        o_out[...] = answer(1)
        o_copy().start()
        attend(0, far)
        attn_ref[...] = answer(0)

    finish_send(r3)

    @pl.when(inner)
    def _():
        finish_send(o2)

    def combine(i, values):
        pick = jnp.where(turned[:, i : i + 1] == slot_lane, 1.0, 0.0).astype(BF16)
        return jnp.dot(pick, values, preferred_element_type=F32) * turned[:, S + i : S + i + 1]

    moe[...] = combine(0, finish(s))
    for i in range(1, S - 1):
        z_return(s, order[i]).wait_recv()
        moe[...] += combine(i, ret[order[i]])

    @pl.when(jnp.logical_not(inner))
    def _():
        o_copy().wait_recv()
        attn_ref[...] = o_in[...]

    z_return(s, order[S - 1]).wait_recv()
    moe_ref[...] = (moe[...] + combine(S - 1, ret[order[S - 1]])).astype(BF16)

    def drain(i, unused):
        to = lax.rem(s + i, S)
        z_copy(to, s).wait_send()
        z_return(to, s).wait_send()
        return unused

    lax.fori_loop(1, S, drain, jnp.int32(0))

    def drain_chunk(i, unused):
        x_forward(i, x).wait_send()
        x_reduce(i).wait_send()
        for origin in range(X):
            t_forward(i, origin, c).wait_send()
            t_reduce(i, origin).wait_send()
        return unused

    lax.fori_loop(0, S, drain_chunk, jnp.int32(0))
    for part in range(2):
        kv_copy(s, part, onward).wait_send()

    @pl.when(inner)
    def _():
        for part in range(2):
            kv_copy(mate, part, facing).wait_send()
        o_copy().wait_send()

    @pl.when(jnp.logical_not(inner))
    def _():
        q_copy().wait_send()


def store_kernel(attn_ref, moe_ref, attn_hbm, moe_hbm, sems):
    stores = [
        pltpu.make_async_copy(attn_ref, attn_hbm, sems.at[0]),
        pltpu.make_async_copy(moe_ref, moe_hbm, sems.at[1]),
    ]
    for store in stores:
        store.start()
    for store in stores:
        store.wait()


def store(attn, moe):
    vmem = pl.BlockSpec(memory_space=pltpu.VMEM)
    hbm = pl.BlockSpec(memory_space=pltpu.HBM)
    return pl.pallas_call(
        store_kernel,
        out_shape=tuple(jax.ShapeDtypeStruct(a.shape, a.dtype) for a in (attn, moe)),
        in_specs=[vmem, vmem],
        out_specs=(hbm, hbm),
        scratch_shapes=[pltpu.SemaphoreType.DMA((2,))],
        compiler_params=pltpu.CompilerParams(vmem_limit_bytes=VMEM_LIMIT // 8),
    )(attn, moe)


def fast_call(S, X, capp, args):
    q, tok, up, flags = args[0], args[6], args[9], args[5]
    width, length = q.shape
    tokens, D = tok.shape
    hidden = up.shape[2]
    hbm = pl.BlockSpec(memory_space=pltpu.HBM)
    vmem = pl.BlockSpec(memory_space=pltpu.VMEM)
    dma = pltpu.SemaphoreType.DMA
    half = pltpu.VMEM((width, length), BF16)
    slots = pltpu.VMEM((S, capp, D), BF16)
    return pl.pallas_call(
        functools.partial(fast_kernel, (S, X, capp)),
        out_shape=(
            jax.ShapeDtypeStruct((width, length), BF16),
            jax.ShapeDtypeStruct((tokens, D), BF16),
        ),
        in_specs=[hbm] * 13,
        out_specs=(vmem, vmem),
        scratch_shapes=[
            half, half, half, half, half,
            pltpu.SMEM(flags.shape, jnp.int32),
            pltpu.VMEM((tokens, D), BF16),
            pltpu.VMEM((2, tokens), jnp.int32),
            pltpu.VMEM((2, tokens), F32),
            pltpu.VMEM((D, hidden), BF16),
            pltpu.VMEM((1, hidden), F32),
            pltpu.VMEM((hidden, D), BF16),
            pltpu.VMEM((1, D), F32),
            slots,
            pltpu.VMEM((S, X, 2, capp, D), BF16),
            pltpu.VMEM((S, X, 2, capp, D), BF16),
            pltpu.VMEM((S, X, capp, D), BF16),
            slots, slots, slots,
            pltpu.VMEM((S, 2, width, length), BF16),
            pltpu.VMEM((S, length, width), BF16),
            half, half, half,
            pltpu.VMEM((2, width // HD, width, length), BF16),
            pltpu.VMEM((2, width, length), F32),
            pltpu.VMEM((2, 2 * width // HD, length), F32),
            pltpu.VMEM((tokens, D), F32),
            pltpu.VMEM((128, tokens), F32),
            dma((13,)),
            dma((S,)), dma((S,)), dma((S,)), dma((S,)), dma((S, X)), dma((S, X)),
            dma((S, X)), dma((S, X)), dma((S,)), dma((S,)), dma((S,)), dma((S,)),
            dma((S, 2)), dma((S, 2)), dma((2,)), dma((2,)),
        ],
        compiler_params=pltpu.CompilerParams(
            collective_id=0, has_side_effects=True, vmem_limit_bytes=VMEM_LIMIT
        ),
    )(*[pltpu.with_memory_space_constraint(a, pltpu.HBM) for a in args])


def local(
    attn_query, fresh_keys, fresh_values, stale_keys, stale_values, block_flags,
    moe_tokens, expert_ids, gate_weights, up_weight, up_bias, down_weight, down_bias,
):
    S, X = lax.axis_size("seq"), lax.axis_size("exp")
    assert lax.axis_size("tp") == 2 and up_weight.shape[0] == 1
    tokens, D = moe_tokens.shape
    length, width = attn_query.shape
    hidden = up_weight.shape[2]
    cap = 5 * tokens // (2 * S)
    capp = -(-cap // 16) * 16
    if (S, X) == (4, 2):
        attn_out, moe_out = fast_call(S, X, capp, (
            attn_query.T, fresh_keys.T, fresh_values.T, stale_keys.T, stale_values.T, block_flags,
            moe_tokens, expert_ids.T, gate_weights.T,
            up_weight, up_bias, down_weight, down_bias,
        ))
        attn_out, moe_out = store(attn_out, moe_out)
        return attn_out.T, moe_out
    vmem = pl.BlockSpec(memory_space=pltpu.VMEM)
    smem = pl.BlockSpec(memory_space=pltpu.SMEM)
    hbm = pl.BlockSpec(memory_space=pl.ANY)
    dma = pltpu.SemaphoreType.DMA
    attn_out, moe_out = pl.pallas_call(
        functools.partial(layer_kernel, (S, X, capp)),
        out_shape=(
            jax.ShapeDtypeStruct((width, length), BF16),
            jax.ShapeDtypeStruct((tokens, D), BF16),
        ),
        in_specs=[vmem] * 5 + [smem] + [vmem] * 3 + [hbm, vmem, hbm, vmem],
        out_specs=(vmem, vmem),
        scratch_shapes=[
            pltpu.VMEM((D, hidden), BF16),
            pltpu.VMEM((hidden, D), BF16),
            pltpu.VMEM((S, tokens), F32),
            pltpu.VMEM((S, capp, D), BF16),
            pltpu.VMEM((S, 2, X, capp, D), BF16),
            pltpu.VMEM((S, X, capp, D), BF16),
            pltpu.VMEM((S, X, capp, D), BF16),
            pltpu.VMEM((S, capp, D), BF16),
            pltpu.VMEM((S, capp, D), BF16),
            pltpu.VMEM((S, 2, width, length), BF16),
            pltpu.VMEM((S * length, width), BF16),
            pltpu.VMEM((width, length), F32),
            pltpu.VMEM((128, tokens), F32),
            dma((2,)),
            dma((S,)), dma((S,)), dma((S, X)), dma((S, X)), dma((S, X)), dma((S, X)),
            dma((S,)), dma((S,)), dma((S, X)), dma((S, X)), dma((S,)), dma((S,)),
            dma((S,)), dma((S,)), dma((S,)),
        ],
        compiler_params=pltpu.CompilerParams(
            collective_id=0, has_side_effects=True, vmem_limit_bytes=67043328
        ),
    )(
        attn_query.T, fresh_keys.T, fresh_values.T, stale_keys.T, stale_values.T, block_flags,
        moe_tokens, expert_ids.T, gate_weights.T,
        up_weight, up_bias, down_weight, down_bias,
    )
    return attn_out.T, moe_out


def solution(mesh):
    in_specs = (
        P(("groups", "seq"), ("exp", "tp")),
        P(("groups", "seq"), ("exp", "tp")),
        P(("groups", "seq"), ("exp", "tp")),
        P(("groups", "seq"), ("exp", "tp")),
        P(("groups", "seq"), ("exp", "tp")),
        P(("groups", "seq")),
        P(("groups", "seq", "exp", "tp"), None),
        P(("groups", "seq", "exp", "tp"), None),
        P(("groups", "seq", "exp", "tp"), None),
        P("seq", None, ("exp", "tp")),
        P("seq", ("exp", "tp")),
        P("seq", ("exp", "tp"), None),
        P("seq", None),
    )
    out_specs = (P(("groups", "seq"), ("exp", "tp")), P(("groups", "seq", "exp", "tp"), None))
    return jax.shard_map(local, mesh=mesh, in_specs=in_specs, out_specs=out_specs, check_vma=False)
```

```python
import functools
import math

import jax
import jax.numpy as jnp
from jax import lax
from jax.experimental import pallas as pl
from jax.experimental.pallas import tpu as pltpu
from jax.sharding import PartitionSpec as P

HD = 72
MESH = pl.DeviceIdType.MESH
F32 = jnp.float32
BF16 = jnp.bfloat16
VMEM_LIMIT = 40 * 1024 * 1024


def layer_kernel(
    sizes,
    q_ref, fresh_k, fresh_v, stale_k, stale_v, flags,
    tok_ref, ids_ref, gate_ref,
    up_hbm, upb_ref, down_hbm, downb_ref,
    attn_ref, moe_ref,
    up_v, down_v, place_v, disp, rows, tpin, xin, fin, ret, kv, keys_v, acc, turn,
    w_sem,
    z_send, z_recv, xf_send, xf_recv, tf_send, tf_recv,
    tr_send, tr_recv, xr_send, xr_recv, zr_send, zr_recv, kv_right, kv_left, kv_recv,
):
    S, X, capp = sizes
    s, x, c = lax.axis_index("seq"), lax.axis_index("exp"), lax.axis_index("tp")
    oc = 1 - c
    T, D = tok_ref.shape
    W, L = q_ref.shape
    heads = W // HD
    blk = L // flags.shape[0]

    up_copy = pltpu.make_async_copy(up_hbm.at[0], up_v, w_sem.at[0])
    down_copy = pltpu.make_async_copy(down_hbm.at[0], down_v, w_sem.at[1])
    up_copy.start()
    down_copy.start()

    def rdma(src, dst, ssem, rsem, where):
        return pltpu.make_async_remote_copy(
            src_ref=src, dst_ref=dst, send_sem=ssem, recv_sem=rsem,
            device_id=where, device_id_type=MESH,
        )

    def z_copy(e, slot):
        return rdma(disp.at[e], rows.at[slot, c, x], z_send.at[e], z_recv.at[slot], {"seq": e})

    def x_forward(src, to, origin):
        return rdma(
            rows.at[src, c, origin], rows.at[src, c, origin],
            xf_send.at[src, to], xf_recv.at[src, origin], {"exp": to},
        )

    def t_forward(src, origin, side):
        return rdma(
            rows.at[src, side, origin], rows.at[src, side, origin],
            tf_send.at[src, origin], tf_recv.at[src, origin], {"tp": oc},
        )

    def t_reduce(src):
        return rdma(rows.at[src, oc], tpin.at[src], tr_send.at[src], tr_recv.at[src], {"tp": oc})

    def x_reduce(src, to, origin):
        return rdma(
            rows.at[src, c, to], xin.at[src, origin],
            xr_send.at[src, to], xr_recv.at[src, origin], {"exp": to},
        )

    def z_return(src, slot):
        return rdma(fin.at[src], ret.at[slot], zr_send.at[src], zr_recv.at[slot], {"seq": src})

    def kv_copy(b, step):
        sems = kv_right if step > 0 else kv_left
        return rdma(kv.at[b], kv.at[b], sems.at[b], kv_recv.at[b], {"seq": s + step})

    def other_x(i):
        return lax.rem(x + i, X)

    def order(k):
        side = jnp.minimum(s, S - 1 - s)
        near = k // 2 + 1
        near = jnp.where(lax.rem(k, 2) == 0, near, -near)
        far = k - side + 1
        far = jnp.where(2 * s < S, far, -far)
        step = jnp.where(k < 2 * side, near, far)
        return s + jnp.where(k == S - 1, 0, step)

    barrier = pltpu.get_barrier_semaphore()
    for i in range(1, S):
        pl.semaphore_signal(barrier, inc=1, device_id={"seq": lax.rem(s + i, S)}, device_id_type=MESH)
    for i in range(1, X):
        pl.semaphore_signal(barrier, inc=1, device_id={"exp": other_x(i)}, device_id_type=MESH)
    pl.semaphore_signal(barrier, inc=1, device_id={"tp": oc}, device_id_type=MESH)

    expert = lax.broadcasted_iota(jnp.int32, (S, T), 0)
    named = (ids_ref[0:1, :] == expert) | (ids_ref[1:2, :] == expert)
    earlier = lax.broadcasted_iota(jnp.int32, (T, T), 0) < lax.broadcasted_iota(jnp.int32, (T, T), 1)
    place = jnp.dot(
        jnp.where(named, 1.0, 0.0).astype(BF16),
        jnp.where(earlier, 1.0, 0.0).astype(BF16),
        preferred_element_type=F32,
    )
    place_v[...] = jnp.where(named, place, -1.0)
    slot_rows = lax.broadcasted_iota(jnp.int32, (capp, T), 0).astype(F32)

    def slots_of(e):
        pick = jnp.where(place_v[pl.ds(e, 1), :] == slot_rows, 1.0, 0.0).astype(BF16)
        return jnp.dot(pick, tok_ref[...], preferred_element_type=F32).astype(BF16)

    def forward(src):
        for i in range(1, X):
            x_forward(src, other_x(i), x).start()
        t_forward(src, x, c).start()

    rows[s, c, x] = slots_of(s)
    pl.semaphore_wait(barrier, S - 1 + X - 1 + 1)
    forward(s)
    def dispatch(k):
        e = order(jnp.int32(k))
        disp[e] = slots_of(e)
        z_copy(e, s).start()

    for k in range(min(2, S - 1)):
        dispatch(k)
    for b in range(flags.shape[0]):
        fresh = flags[b] == 1
        part = pl.ds(b * blk, blk)
        kv[s, 0, :, part] = jnp.where(fresh, fresh_k[:, part], stale_k[:, part])
        kv[s, 1, :, part] = jnp.where(fresh, fresh_v[:, part], stale_v[:, part])

    def relay(step):
        low, high = s - (step - 1), s + (step - 1)

        @pl.when(low >= 0)
        def _():
            @pl.when(low < s)
            def _():
                kv_copy(low, 1).wait_recv()

            @pl.when(s + 1 < S)
            def _():
                kv_copy(low, 1).start()

        @pl.when(high < S)
        def _():
            @pl.when(high > s)
            def _():
                kv_copy(high, -1).wait_recv()

            @pl.when(s - 1 >= 0)
            def _():
                kv_copy(high, -1).start()

    relay(1)
    for k in range(2, S - 1):
        dispatch(k)
    nearest = order(jnp.int32(0))
    z_copy(nearest, nearest).wait_recv()
    forward(nearest)

    up_copy.wait()
    down_copy.wait()

    def finish(src):
        total = rows[src, c, x].astype(F32) + downb_ref[...]
        for i in range(1, X):
            x_reduce(src, other_x(i), other_x(i)).wait_recv()
            total = total + xin[src, other_x(i)].astype(F32)
        done = total.astype(BF16)
        fin[src] = done

    def finish_send(src):
        finish(src)

        @pl.when(src != s)
        def _():
            z_return(src, s).start()

        @pl.when(src == s)
        def _():
            ret[s] = fin[s]

    def chunk(k, unused):
        src = order(k)
        for i in range(1, X):
            x_forward(src, other_x(i), other_x(i)).wait_recv()
            t_forward(src, other_x(i), c).start()

        @pl.when(k + 1 < S - 1)
        def _():
            nxt = order(k + 1)
            z_copy(nxt, nxt).wait_recv()
            forward(nxt)

        for i in range(X):
            t_forward(src, other_x(i), oc).wait_recv()
        for i in range(1, X):
            x_forward(src, other_x(i), x).wait_send()
        for i in range(X):
            t_forward(src, other_x(i), c).wait_send()

        block = rows[src].reshape(2 * X * capp, D)
        hidden = jnp.dot(block, up_v[...], preferred_element_type=F32) + upb_ref[...]
        hidden = jax.nn.gelu(hidden).astype(BF16)
        result = jnp.dot(hidden, down_v[...], preferred_element_type=F32).astype(BF16)
        rows[src] = result.reshape(2, X, capp, D)
        t_reduce(src).start()

        @pl.when(k >= 1)
        def _():
            finish_send(order(k - 1))

        @pl.when(k == 0)
        def _():
            relay(2)

        @pl.when((k >= 2) & (k < S - 1))
        def _():
            relay(k + 1)

        t_reduce(src).wait_recv()
        for i in range(X):
            to = other_x(i)
            rows[src, c, to] = (rows[src, c, to].astype(F32) + tpin[src, to].astype(F32)).astype(BF16)
            if i > 0:
                x_reduce(src, to, x).start()
        return unused

    lax.fori_loop(0, S, chunk, jnp.int32(0))

    relay(S)

    for i in range(S):
        keys_v[pl.ds(i * L, L), :] = kv[i, 0].T
    scale = 1.0 / math.sqrt(HD)
    channel = lax.broadcasted_iota(jnp.int32, (W, L), 0)

    def head(h, unused):
        mine = (channel >= h * HD) & (channel < (h + 1) * HD)
        query = jnp.where(mine, q_ref[...].astype(F32), 0.0).astype(BF16)
        scores = jnp.dot(keys_v[...], query, preferred_element_type=F32) * scale
        probs = jnp.exp(scores - jnp.max(scores, axis=0, keepdims=True))
        total = jnp.sum(probs, axis=0, keepdims=True)
        weights = probs.astype(BF16)
        mixed = jnp.zeros((W, L), F32)
        for i in range(S):
            mixed += jnp.dot(kv[i, 1], weights[i * L : (i + 1) * L], preferred_element_type=F32)
        acc[...] = jnp.where(mine, mixed / total, acc[...])
        return unused

    acc[...] = jnp.zeros_like(acc)
    lax.fori_loop(0, heads, head, jnp.int32(0))
    attn_ref[...] = acc[...].astype(BF16)
    finish_send(s)

    base = jnp.where(named, place, 0.0) + (expert * capp).astype(F32)
    turn[...] = jnp.zeros_like(turn)
    for j in range(2):
        hit = ids_ref[j : j + 1, :] == expert
        turn[j : j + 1, :] = jnp.sum(jnp.where(hit, base, 0.0), axis=0, keepdims=True)
        turn[2 + j : 3 + j, :] = gate_ref[j : j + 1, :]
    turned = turn[...].T
    slot_lane = lax.broadcasted_iota(jnp.int32, (T, S * capp), 1).astype(F32)
    picks = [jnp.where(turned[:, j : j + 1] == slot_lane, 1.0, 0.0).astype(BF16) for j in range(2)]
    for i in range(1, S):
        z_return(s, lax.rem(s + i, S)).wait_recv()
    everything = ret[...].reshape(S * capp, D)
    moe_ref[...] = (
        jnp.dot(picks[0], everything, preferred_element_type=F32) * turned[:, 2:3]
        + jnp.dot(picks[1], everything, preferred_element_type=F32) * turned[:, 3:4]
    ).astype(BF16)

    def drain(i, unused):
        to = lax.rem(s + i, S)
        z_copy(to, s).wait_send()
        z_return(to, s).wait_send()
        return unused

    lax.fori_loop(1, S, drain, jnp.int32(0))

    def drain_chunk(i, unused):
        t_reduce(i).wait_send()
        for j in range(1, X):
            x_reduce(i, other_x(j), x).wait_send()

        @pl.when((i <= s) & (s + 1 < S))
        def _():
            kv_copy(i, 1).wait_send()

        @pl.when((i >= s) & (s - 1 >= 0))
        def _():
            kv_copy(i, -1).wait_send()

        return unused

    lax.fori_loop(0, S, drain_chunk, jnp.int32(0))


def fast_kernel(
    sizes,
    q_hbm, fk_hbm, fv_hbm, sk_hbm, sv_hbm, flags_hbm, tok_hbm, ids_hbm, gate_hbm,
    up_hbm, upb_hbm, down_hbm, downb_hbm,
    attn_ref, moe_ref,
    q_v, fresh_k, fresh_v, stale_k, stale_v, flags, tok_v, ids_v, gate_v,
    up_v, upb_v, down_v, downb_v,
    disp, rows, outs, tpin, xin, fin, ret, kv, keys_v, q_in, o_out, o_in, masked, acc, stat, moe, turn,
    in_sem,
    z_send, z_recv, xf_send, xf_recv, tf_send, tf_recv,
    tr_send, tr_recv, xr_send, xr_recv, zr_send, zr_recv, kv_send, kv_recv, qo_send, qo_recv,
):
    S, X, capp = sizes
    s, x, c = lax.axis_index("seq"), lax.axis_index("exp"), lax.axis_index("tp")
    oc, ox = 1 - c, 1 - x
    T, D = tok_v.shape
    W, L = q_v.shape
    heads = W // HD
    blocks = flags.shape[0]
    blk = L // blocks

    barrier = pltpu.get_barrier_semaphore()
    for i in range(1, S):
        pl.semaphore_signal(barrier, inc=1, device_id={"seq": lax.rem(s + i, S)}, device_id_type=MESH)
    pl.semaphore_signal(barrier, inc=1, device_id={"exp": ox}, device_id_type=MESH)
    pl.semaphore_signal(barrier, inc=1, device_id={"tp": oc}, device_id_type=MESH)

    pairs = (
        (ids_hbm, ids_v), (tok_hbm, tok_v), (flags_hbm, flags),
        (fk_hbm, fresh_k), (sk_hbm, stale_k), (fv_hbm, fresh_v), (sv_hbm, stale_v),
        (up_hbm.at[0], up_v), (upb_hbm, upb_v), (down_hbm.at[0], down_v), (downb_hbm, downb_v),
        (q_hbm, q_v), (gate_hbm, gate_v),
    )
    loads = [pltpu.make_async_copy(a, b, in_sem.at[i]) for i, (a, b) in enumerate(pairs)]
    for load in loads:
        load.start()

    def rdma(src, dst, ssem, rsem, where):
        return pltpu.make_async_remote_copy(
            src_ref=src, dst_ref=dst, send_sem=ssem, recv_sem=rsem,
            device_id=where, device_id_type=MESH,
        )

    def z_copy(e, slot):
        return rdma(disp.at[e], rows.at[slot, x, c], z_send.at[e], z_recv.at[slot], {"seq": e})

    def x_forward(src, origin):
        return rdma(
            rows.at[src, origin, c], rows.at[src, origin, c],
            xf_send.at[src], xf_recv.at[src], {"exp": ox},
        )

    def t_forward(src, origin, side):
        return rdma(
            rows.at[src, origin, side], rows.at[src, origin, side],
            tf_send.at[src, origin], tf_recv.at[src, origin], {"tp": oc},
        )

    def t_reduce(src, origin):
        return rdma(
            outs.at[src, origin, oc], tpin.at[src, origin],
            tr_send.at[src, origin], tr_recv.at[src, origin], {"tp": oc},
        )

    def x_reduce(src):
        return rdma(outs.at[src, ox, c], xin.at[src], xr_send.at[src], xr_recv.at[src], {"exp": ox})

    def z_return(src, slot):
        return rdma(fin.at[src], ret.at[slot], zr_send.at[src], zr_recv.at[slot], {"seq": src})

    mate, facing = s + 1 - 2 * lax.rem(s, 2), S - 1 - s
    far = S - 1 - mate
    inner = (s != 0) & (s != S - 1)

    def kv_copy(b, part, to):
        return rdma(kv.at[b, part], kv.at[b, part], kv_send.at[b, part], kv_recv.at[b, part], {"seq": to})

    def q_copy():
        return rdma(q_v, q_in, qo_send.at[0], qo_recv.at[0], {"seq": mate})

    def o_copy():
        return rdma(o_out, o_in, qo_send.at[1], qo_recv.at[1], {"seq": mate})

    def mirrored(end, inner):
        near = jnp.where((s == 0) | (s == S - 1), end, inner)
        return jnp.where(2 * s < S, near, S - 1 - near)

    targets = [mirrored(a, b) for a, b in ((1, 2), (S - 1, 0), (2, S - 1))]
    order = [s, mate, facing, far]

    loads[0].wait()
    loads[1].wait()
    expert = lax.broadcasted_iota(jnp.int32, (S, T), 0)
    named = (ids_v[0:1, :] == expert) | (ids_v[1:2, :] == expert)
    earlier = lax.broadcasted_iota(jnp.int32, (T, T), 0) < lax.broadcasted_iota(jnp.int32, (T, T), 1)
    place = jnp.dot(
        jnp.where(named, 1.0, 0.0).astype(BF16),
        jnp.where(earlier, 1.0, 0.0).astype(BF16),
        preferred_element_type=F32,
    )
    slotted = jnp.where(named, place, -1.0)
    slot_rows = lax.broadcasted_iota(jnp.int32, (capp, T), 0).astype(F32)
    for e in range(S):
        pick = jnp.where(slotted[e : e + 1, :] == slot_rows, 1.0, 0.0).astype(BF16)
        disp[e] = jnp.dot(pick, tok_v[...], preferred_element_type=F32).astype(BF16)
    rows[s, x, c] = disp[s]
    for load in loads[2:7]:
        load.wait()
    for b in range(blocks):
        fresh = flags[b] == 1
        part = pl.ds(b * blk, blk)
        kv[s, 0, :, part] = jnp.where(fresh, fresh_k[:, part], stale_k[:, part])
        kv[s, 1, :, part] = jnp.where(fresh, fresh_v[:, part], stale_v[:, part])

    pl.semaphore_wait(barrier, S - 1 + 1 + 1)

    def forward(src):
        x_forward(src, x).start()
        t_forward(src, x, c).start()

    def arrive(src):
        z_copy(src, src).wait_recv()
        forward(src)

    for e in targets:
        z_copy(e, s).start()
    forward(s)

    onward = jnp.where(inner, facing, mate)
    kv_copy(s, 0, onward).start()
    kv_copy(s, 1, onward).start()

    for load in loads[7:]:
        load.wait()

    @pl.when(jnp.logical_not(inner))
    def _():
        q_copy().start()

    scale = 1.0 / math.sqrt(HD)
    channel = lax.broadcasted_iota(jnp.int32, (W, L), 0)

    def ask(i, source):
        for h in range(heads):
            own = (channel >= h * HD) & (channel < (h + 1) * HD)
            masked[i, h] = jnp.where(own, source[...].astype(F32), 0.0).astype(BF16)

    def take(b):
        keys_v[b] = kv[b, 0].T

    def attend(i, b, first=False):
        for h in range(heads):
            lo, hi = h * HD, (h + 1) * HD
            a, z = lo // 128 * 128, min(-(-hi // 128) * 128, W)
            scores = jnp.dot(keys_v[b, :, a:z], masked[i, h, a:z, :], preferred_element_type=F32) * scale
            top = jnp.max(scores, axis=0, keepdims=True)
            if not first:
                before = stat[i, h : h + 1, :]
                top = jnp.maximum(before, top)
                fade = jnp.exp(before - top)
            probs = jnp.exp(scores - top)
            total = jnp.sum(probs, axis=0, keepdims=True)
            a, z = lo // 16 * 16, -(-hi // 16) * 16
            mixed = jnp.dot(kv[b, 1, a:z, :], probs.astype(BF16), preferred_element_type=F32)
            mixed = mixed[lo - a : hi - a]
            if not first:
                total = stat[i, heads + h : heads + h + 1, :] * fade + total
                mixed = acc[i, lo:hi, :] * fade + mixed
            stat[i, h : h + 1, :] = top
            stat[i, heads + h : heads + h + 1, :] = total
            acc[i, lo:hi, :] = mixed

    def answer(i):
        for h in range(heads):
            lo, hi = h * HD, (h + 1) * HD
            acc[i, lo:hi, :] = acc[i, lo:hi, :] / stat[i, heads + h : heads + h + 1, :]
        return acc[i].astype(BF16)

    def mlp(src, origin):
        block = rows[src, origin].reshape(2 * capp, D)
        hidden = jnp.dot(block, up_v[...], preferred_element_type=F32) + upb_v[...]
        hidden = jax.nn.gelu(hidden).astype(BF16)
        result = jnp.dot(hidden, down_v[...], preferred_element_type=F32).astype(BF16)
        outs[src, origin] = result.reshape(2, capp, D)
        t_reduce(src, origin).start()

    def mine(src):
        t_forward(src, x, oc).wait_recv()
        mlp(src, x)

    def crossed(src):
        x_forward(src, ox).wait_recv()
        t_forward(src, ox, c).start()

    def other(src):
        t_forward(src, ox, oc).wait_recv()
        mlp(src, ox)

    def reduce(src):
        t_reduce(src, ox).wait_recv()
        outs[src, ox, c] = (outs[src, ox, c].astype(F32) + tpin[src, ox].astype(F32)).astype(BF16)
        x_reduce(src).start()

    def finish(src):
        t_reduce(src, x).wait_recv()
        total = outs[src, x, c].astype(F32) + tpin[src, x].astype(F32) + downb_v[...]
        x_reduce(src).wait_recv()
        return (total + xin[src].astype(F32)).astype(BF16)

    def finish_send(src):
        fin[src] = finish(src)
        z_return(src, s).start()

    o0, o1, o2, o3 = order
    landing = [s, mate, jnp.where(inner, far, facing), jnp.where(inner, facing, far)]
    mine(o0)
    turn[...] = jnp.zeros_like(turn)
    for i, e in enumerate(landing):
        hit = [ids_v[j : j + 1, :] == e for j in range(2)]
        spot = jnp.sum(jnp.where(expert == e, place, 0.0), axis=0, keepdims=True)
        turn[i : i + 1, :] = jnp.where(hit[0] | hit[1], spot, -1.0)
        turn[S + i : S + i + 1, :] = sum(
            jnp.where(hit[j], gate_v[j : j + 1, :], 0.0) for j in range(2)
        )
    turned = turn[...].T
    slot_lane = lax.broadcasted_iota(jnp.int32, (T, capp), 1).astype(F32)

    outer = jnp.logical_not(inner)
    r1, r3 = jnp.where(inner, o1, o2), jnp.where(inner, o3, o1)

    @pl.when(inner)
    def _():
        ask(0, q_v)
        take(s)
        attend(0, s, first=True)

    arrive(o1)

    @pl.when(inner)
    def _():
        arrive(o2)

    crossed(o0)
    mine(o1)
    other(o0)
    crossed(o1)

    @pl.when(outer)
    def _():
        arrive(o2)

    other(o1)
    mine(o2)

    @pl.when(outer)
    def _():
        arrive(o3)

    crossed(o2)

    @pl.when(inner)
    def _():
        arrive(o3)
        reduce(o1)
        kv_copy(mate, 0, mate).wait_recv()
        kv_copy(mate, 0, facing).start()

    other(o2)
    mine(o3)
    reduce(o2)

    @pl.when(inner)
    def _():
        kv_copy(mate, 1, mate).wait_recv()
        kv_copy(mate, 1, facing).start()
        take(mate)

    crossed(o3)

    @pl.when(inner)
    def _():
        attend(0, mate)

    other(o3)

    @pl.when(inner)
    def _():
        q_copy().wait_recv()
        ask(1, q_in)
        attend(1, s, first=True)

    reduce(o3)

    @pl.when(outer)
    def _():
        reduce(o1)

    reduce(o0)
    finish_send(r1)

    @pl.when(inner)
    def _():
        attend(1, mate)
        kv_copy(facing, 0, facing).wait_recv()
        kv_copy(facing, 1, facing).wait_recv()
        take(facing)
        attend(1, facing)
        attend(0, facing)

    @pl.when(outer)
    def _():
        finish_send(o3)

    @pl.when(inner & (c == 1))
    def _():
        finish_send(o2)

    @pl.when(inner)
    def _():
        kv_copy(far, 0, facing).wait_recv()
        kv_copy(far, 1, facing).wait_recv()
        take(far)
        attend(1, far)
        o_out[...] = answer(1)
        o_copy().start()
        attend(0, far)
        attn_ref[...] = answer(0)

    finish_send(r3)

    @pl.when(inner & (c == 0))
    def _():
        finish_send(o2)

    def combine(i, values):
        pick = jnp.where(turned[:, i : i + 1] == slot_lane, 1.0, 0.0).astype(BF16)
        return jnp.dot(pick, values, preferred_element_type=F32) * turned[:, S + i : S + i + 1]

    moe[...] = combine(0, finish(s))
    for i in range(1, S - 1):
        z_return(s, landing[i]).wait_recv()
        moe[...] += combine(i, ret[landing[i]])

    @pl.when(jnp.logical_not(inner))
    def _():
        o_copy().wait_recv()
        attn_ref[...] = o_in[...]

    z_return(s, landing[S - 1]).wait_recv()
    moe_ref[...] = (moe[...] + combine(S - 1, ret[landing[S - 1]])).astype(BF16)

    def drain(i, unused):
        to = lax.rem(s + i, S)
        z_copy(to, s).wait_send()
        z_return(to, s).wait_send()
        return unused

    lax.fori_loop(1, S, drain, jnp.int32(0))

    def drain_chunk(i, unused):
        x_forward(i, x).wait_send()
        x_reduce(i).wait_send()
        for origin in range(X):
            t_forward(i, origin, c).wait_send()
            t_reduce(i, origin).wait_send()
        return unused

    lax.fori_loop(0, S, drain_chunk, jnp.int32(0))
    for part in range(2):
        kv_copy(s, part, onward).wait_send()

    @pl.when(inner)
    def _():
        for part in range(2):
            kv_copy(mate, part, facing).wait_send()
        o_copy().wait_send()

    @pl.when(jnp.logical_not(inner))
    def _():
        q_copy().wait_send()


def store_kernel(attn_ref, moe_ref, attn_hbm, moe_hbm, sems):
    stores = [
        pltpu.make_async_copy(attn_ref, attn_hbm, sems.at[0]),
        pltpu.make_async_copy(moe_ref, moe_hbm, sems.at[1]),
    ]
    for store in stores:
        store.start()
    for store in stores:
        store.wait()


def store(attn, moe):
    vmem = pl.BlockSpec(memory_space=pltpu.VMEM)
    hbm = pl.BlockSpec(memory_space=pltpu.HBM)
    return pl.pallas_call(
        store_kernel,
        out_shape=tuple(jax.ShapeDtypeStruct(a.shape, a.dtype) for a in (attn, moe)),
        in_specs=[vmem, vmem],
        out_specs=(hbm, hbm),
        scratch_shapes=[pltpu.SemaphoreType.DMA((2,))],
        compiler_params=pltpu.CompilerParams(vmem_limit_bytes=VMEM_LIMIT // 8),
    )(attn, moe)


def fast_call(S, X, capp, args):
    q, tok, up, flags = args[0], args[6], args[9], args[5]
    width, length = q.shape
    tokens, D = tok.shape
    hidden = up.shape[2]
    hbm = pl.BlockSpec(memory_space=pltpu.HBM)
    vmem = pl.BlockSpec(memory_space=pltpu.VMEM)
    dma = pltpu.SemaphoreType.DMA
    half = pltpu.VMEM((width, length), BF16)
    slots = pltpu.VMEM((S, capp, D), BF16)
    return pl.pallas_call(
        functools.partial(fast_kernel, (S, X, capp)),
        out_shape=(
            jax.ShapeDtypeStruct((width, length), BF16),
            jax.ShapeDtypeStruct((tokens, D), BF16),
        ),
        in_specs=[hbm] * 13,
        out_specs=(vmem, vmem),
        scratch_shapes=[
            half, half, half, half, half,
            pltpu.SMEM(flags.shape, jnp.int32),
            pltpu.VMEM((tokens, D), BF16),
            pltpu.VMEM((2, tokens), jnp.int32),
            pltpu.VMEM((2, tokens), F32),
            pltpu.VMEM((D, hidden), BF16),
            pltpu.VMEM((1, hidden), F32),
            pltpu.VMEM((hidden, D), BF16),
            pltpu.VMEM((1, D), F32),
            slots,
            pltpu.VMEM((S, X, 2, capp, D), BF16),
            pltpu.VMEM((S, X, 2, capp, D), BF16),
            pltpu.VMEM((S, X, capp, D), BF16),
            slots, slots, slots,
            pltpu.VMEM((S, 2, width, length), BF16),
            pltpu.VMEM((S, length, width), BF16),
            half, half, half,
            pltpu.VMEM((2, width // HD, width, length), BF16),
            pltpu.VMEM((2, width, length), F32),
            pltpu.VMEM((2, 2 * width // HD, length), F32),
            pltpu.VMEM((tokens, D), F32),
            pltpu.VMEM((128, tokens), F32),
            dma((13,)),
            dma((S,)), dma((S,)), dma((S,)), dma((S,)), dma((S, X)), dma((S, X)),
            dma((S, X)), dma((S, X)), dma((S,)), dma((S,)), dma((S,)), dma((S,)),
            dma((S, 2)), dma((S, 2)), dma((2,)), dma((2,)),
        ],
        compiler_params=pltpu.CompilerParams(
            collective_id=0, has_side_effects=True, vmem_limit_bytes=VMEM_LIMIT
        ),
    )(*[pltpu.with_memory_space_constraint(a, pltpu.HBM) for a in args])


def local(
    attn_query, fresh_keys, fresh_values, stale_keys, stale_values, block_flags,
    moe_tokens, expert_ids, gate_weights, up_weight, up_bias, down_weight, down_bias,
):
    S, X = lax.axis_size("seq"), lax.axis_size("exp")
    assert lax.axis_size("tp") == 2 and up_weight.shape[0] == 1
    tokens, D = moe_tokens.shape
    length, width = attn_query.shape
    hidden = up_weight.shape[2]
    cap = 5 * tokens // (2 * S)
    capp = -(-cap // 16) * 16
    if (S, X) == (4, 2):
        attn_out, moe_out = fast_call(S, X, capp, (
            attn_query.T, fresh_keys.T, fresh_values.T, stale_keys.T, stale_values.T, block_flags,
            moe_tokens, expert_ids.T, gate_weights.T,
            up_weight, up_bias, down_weight, down_bias,
        ))
        attn_out, moe_out = store(attn_out, moe_out)
        return attn_out.T, moe_out
    vmem = pl.BlockSpec(memory_space=pltpu.VMEM)
    smem = pl.BlockSpec(memory_space=pltpu.SMEM)
    hbm = pl.BlockSpec(memory_space=pl.ANY)
    dma = pltpu.SemaphoreType.DMA
    attn_out, moe_out = pl.pallas_call(
        functools.partial(layer_kernel, (S, X, capp)),
        out_shape=(
            jax.ShapeDtypeStruct((width, length), BF16),
            jax.ShapeDtypeStruct((tokens, D), BF16),
        ),
        in_specs=[vmem] * 5 + [smem] + [vmem] * 3 + [hbm, vmem, hbm, vmem],
        out_specs=(vmem, vmem),
        scratch_shapes=[
            pltpu.VMEM((D, hidden), BF16),
            pltpu.VMEM((hidden, D), BF16),
            pltpu.VMEM((S, tokens), F32),
            pltpu.VMEM((S, capp, D), BF16),
            pltpu.VMEM((S, 2, X, capp, D), BF16),
            pltpu.VMEM((S, X, capp, D), BF16),
            pltpu.VMEM((S, X, capp, D), BF16),
            pltpu.VMEM((S, capp, D), BF16),
            pltpu.VMEM((S, capp, D), BF16),
            pltpu.VMEM((S, 2, width, length), BF16),
            pltpu.VMEM((S * length, width), BF16),
            pltpu.VMEM((width, length), F32),
            pltpu.VMEM((128, tokens), F32),
            dma((2,)),
            dma((S,)), dma((S,)), dma((S, X)), dma((S, X)), dma((S, X)), dma((S, X)),
            dma((S,)), dma((S,)), dma((S, X)), dma((S, X)), dma((S,)), dma((S,)),
            dma((S,)), dma((S,)), dma((S,)),
        ],
        compiler_params=pltpu.CompilerParams(
            collective_id=0, has_side_effects=True, vmem_limit_bytes=67043328
        ),
    )(
        attn_query.T, fresh_keys.T, fresh_values.T, stale_keys.T, stale_values.T, block_flags,
        moe_tokens, expert_ids.T, gate_weights.T,
        up_weight, up_bias, down_weight, down_bias,
    )
    return attn_out.T, moe_out


def solution(mesh):
    in_specs = (
        P(("groups", "seq"), ("exp", "tp")),
        P(("groups", "seq"), ("exp", "tp")),
        P(("groups", "seq"), ("exp", "tp")),
        P(("groups", "seq"), ("exp", "tp")),
        P(("groups", "seq"), ("exp", "tp")),
        P(("groups", "seq")),
        P(("groups", "seq", "exp", "tp"), None),
        P(("groups", "seq", "exp", "tp"), None),
        P(("groups", "seq", "exp", "tp"), None),
        P("seq", None, ("exp", "tp")),
        P("seq", ("exp", "tp")),
        P("seq", ("exp", "tp"), None),
        P("seq", None),
    )
    out_specs = (P(("groups", "seq"), ("exp", "tp")), P(("groups", "seq", "exp", "tp"), None))
    return jax.shard_map(local, mesh=mesh, in_specs=in_specs, out_specs=out_specs, check_vma=False)
```

```python
import functools
import math

import jax
import jax.numpy as jnp
from jax import lax
from jax.experimental import pallas as pl
from jax.experimental.pallas import tpu as pltpu
from jax.sharding import PartitionSpec as P

HD = 72
MESH = pl.DeviceIdType.MESH
F32 = jnp.float32
BF16 = jnp.bfloat16
VMEM_LIMIT = 40 * 1024 * 1024


def layer_kernel(
    sizes,
    q_ref, fresh_k, fresh_v, stale_k, stale_v, flags,
    tok_ref, ids_ref, gate_ref,
    up_hbm, upb_ref, down_hbm, downb_ref,
    attn_ref, moe_ref,
    up_v, down_v, place_v, disp, rows, tpin, xin, fin, ret, kv, keys_v, acc, turn,
    w_sem,
    z_send, z_recv, xf_send, xf_recv, tf_send, tf_recv,
    tr_send, tr_recv, xr_send, xr_recv, zr_send, zr_recv, kv_right, kv_left, kv_recv,
):
    S, X, capp = sizes
    s, x, c = lax.axis_index("seq"), lax.axis_index("exp"), lax.axis_index("tp")
    oc = 1 - c
    T, D = tok_ref.shape
    W, L = q_ref.shape
    heads = W // HD
    blk = L // flags.shape[0]

    up_copy = pltpu.make_async_copy(up_hbm.at[0], up_v, w_sem.at[0])
    down_copy = pltpu.make_async_copy(down_hbm.at[0], down_v, w_sem.at[1])
    up_copy.start()
    down_copy.start()

    def rdma(src, dst, ssem, rsem, where):
        return pltpu.make_async_remote_copy(
            src_ref=src, dst_ref=dst, send_sem=ssem, recv_sem=rsem,
            device_id=where, device_id_type=MESH,
        )

    def z_copy(e, slot):
        return rdma(disp.at[e], rows.at[slot, c, x], z_send.at[e], z_recv.at[slot], {"seq": e})

    def x_forward(src, to, origin):
        return rdma(
            rows.at[src, c, origin], rows.at[src, c, origin],
            xf_send.at[src, to], xf_recv.at[src, origin], {"exp": to},
        )

    def t_forward(src, origin, side):
        return rdma(
            rows.at[src, side, origin], rows.at[src, side, origin],
            tf_send.at[src, origin], tf_recv.at[src, origin], {"tp": oc},
        )

    def t_reduce(src):
        return rdma(rows.at[src, oc], tpin.at[src], tr_send.at[src], tr_recv.at[src], {"tp": oc})

    def x_reduce(src, to, origin):
        return rdma(
            rows.at[src, c, to], xin.at[src, origin],
            xr_send.at[src, to], xr_recv.at[src, origin], {"exp": to},
        )

    def z_return(src, slot):
        return rdma(fin.at[src], ret.at[slot], zr_send.at[src], zr_recv.at[slot], {"seq": src})

    def kv_copy(b, step):
        sems = kv_right if step > 0 else kv_left
        return rdma(kv.at[b], kv.at[b], sems.at[b], kv_recv.at[b], {"seq": s + step})

    def other_x(i):
        return lax.rem(x + i, X)

    def order(k):
        side = jnp.minimum(s, S - 1 - s)
        near = k // 2 + 1
        near = jnp.where(lax.rem(k, 2) == 0, near, -near)
        far = k - side + 1
        far = jnp.where(2 * s < S, far, -far)
        step = jnp.where(k < 2 * side, near, far)
        return s + jnp.where(k == S - 1, 0, step)

    barrier = pltpu.get_barrier_semaphore()
    for i in range(1, S):
        pl.semaphore_signal(barrier, inc=1, device_id={"seq": lax.rem(s + i, S)}, device_id_type=MESH)
    for i in range(1, X):
        pl.semaphore_signal(barrier, inc=1, device_id={"exp": other_x(i)}, device_id_type=MESH)
    pl.semaphore_signal(barrier, inc=1, device_id={"tp": oc}, device_id_type=MESH)

    expert = lax.broadcasted_iota(jnp.int32, (S, T), 0)
    named = (ids_ref[0:1, :] == expert) | (ids_ref[1:2, :] == expert)
    earlier = lax.broadcasted_iota(jnp.int32, (T, T), 0) < lax.broadcasted_iota(jnp.int32, (T, T), 1)
    place = jnp.dot(
        jnp.where(named, 1.0, 0.0).astype(BF16),
        jnp.where(earlier, 1.0, 0.0).astype(BF16),
        preferred_element_type=F32,
    )
    place_v[...] = jnp.where(named, place, -1.0)
    slot_rows = lax.broadcasted_iota(jnp.int32, (capp, T), 0).astype(F32)

    def slots_of(e):
        pick = jnp.where(place_v[pl.ds(e, 1), :] == slot_rows, 1.0, 0.0).astype(BF16)
        return jnp.dot(pick, tok_ref[...], preferred_element_type=F32).astype(BF16)

    def forward(src):
        for i in range(1, X):
            x_forward(src, other_x(i), x).start()
        t_forward(src, x, c).start()

    rows[s, c, x] = slots_of(s)
    pl.semaphore_wait(barrier, S - 1 + X - 1 + 1)
    forward(s)
    def dispatch(k):
        e = order(jnp.int32(k))
        disp[e] = slots_of(e)
        z_copy(e, s).start()

    for k in range(min(2, S - 1)):
        dispatch(k)
    for b in range(flags.shape[0]):
        fresh = flags[b] == 1
        part = pl.ds(b * blk, blk)
        kv[s, 0, :, part] = jnp.where(fresh, fresh_k[:, part], stale_k[:, part])
        kv[s, 1, :, part] = jnp.where(fresh, fresh_v[:, part], stale_v[:, part])

    def relay(step):
        low, high = s - (step - 1), s + (step - 1)

        @pl.when(low >= 0)
        def _():
            @pl.when(low < s)
            def _():
                kv_copy(low, 1).wait_recv()

            @pl.when(s + 1 < S)
            def _():
                kv_copy(low, 1).start()

        @pl.when(high < S)
        def _():
            @pl.when(high > s)
            def _():
                kv_copy(high, -1).wait_recv()

            @pl.when(s - 1 >= 0)
            def _():
                kv_copy(high, -1).start()

    relay(1)
    for k in range(2, S - 1):
        dispatch(k)
    nearest = order(jnp.int32(0))
    z_copy(nearest, nearest).wait_recv()
    forward(nearest)

    up_copy.wait()
    down_copy.wait()

    def finish(src):
        total = rows[src, c, x].astype(F32) + downb_ref[...]
        for i in range(1, X):
            x_reduce(src, other_x(i), other_x(i)).wait_recv()
            total = total + xin[src, other_x(i)].astype(F32)
        done = total.astype(BF16)
        fin[src] = done

    def finish_send(src):
        finish(src)

        @pl.when(src != s)
        def _():
            z_return(src, s).start()

        @pl.when(src == s)
        def _():
            ret[s] = fin[s]

    def chunk(k, unused):
        src = order(k)
        for i in range(1, X):
            x_forward(src, other_x(i), other_x(i)).wait_recv()
            t_forward(src, other_x(i), c).start()

        @pl.when(k + 1 < S - 1)
        def _():
            nxt = order(k + 1)
            z_copy(nxt, nxt).wait_recv()
            forward(nxt)

        for i in range(X):
            t_forward(src, other_x(i), oc).wait_recv()
        for i in range(1, X):
            x_forward(src, other_x(i), x).wait_send()
        for i in range(X):
            t_forward(src, other_x(i), c).wait_send()

        block = rows[src].reshape(2 * X * capp, D)
        hidden = jnp.dot(block, up_v[...], preferred_element_type=F32) + upb_ref[...]
        hidden = jax.nn.gelu(hidden).astype(BF16)
        result = jnp.dot(hidden, down_v[...], preferred_element_type=F32).astype(BF16)
        rows[src] = result.reshape(2, X, capp, D)
        t_reduce(src).start()

        @pl.when(k >= 1)
        def _():
            finish_send(order(k - 1))

        @pl.when(k == 0)
        def _():
            relay(2)

        @pl.when((k >= 2) & (k < S - 1))
        def _():
            relay(k + 1)

        t_reduce(src).wait_recv()
        for i in range(X):
            to = other_x(i)
            rows[src, c, to] = (rows[src, c, to].astype(F32) + tpin[src, to].astype(F32)).astype(BF16)
            if i > 0:
                x_reduce(src, to, x).start()
        return unused

    lax.fori_loop(0, S, chunk, jnp.int32(0))

    relay(S)

    for i in range(S):
        keys_v[pl.ds(i * L, L), :] = kv[i, 0].T
    scale = 1.0 / math.sqrt(HD)
    channel = lax.broadcasted_iota(jnp.int32, (W, L), 0)

    def head(h, unused):
        mine = (channel >= h * HD) & (channel < (h + 1) * HD)
        query = jnp.where(mine, q_ref[...].astype(F32), 0.0).astype(BF16)
        scores = jnp.dot(keys_v[...], query, preferred_element_type=F32) * scale
        probs = jnp.exp(scores - jnp.max(scores, axis=0, keepdims=True))
        total = jnp.sum(probs, axis=0, keepdims=True)
        weights = probs.astype(BF16)
        mixed = jnp.zeros((W, L), F32)
        for i in range(S):
            mixed += jnp.dot(kv[i, 1], weights[i * L : (i + 1) * L], preferred_element_type=F32)
        acc[...] = jnp.where(mine, mixed / total, acc[...])
        return unused

    acc[...] = jnp.zeros_like(acc)
    lax.fori_loop(0, heads, head, jnp.int32(0))
    attn_ref[...] = acc[...].astype(BF16)
    finish_send(s)

    base = jnp.where(named, place, 0.0) + (expert * capp).astype(F32)
    turn[...] = jnp.zeros_like(turn)
    for j in range(2):
        hit = ids_ref[j : j + 1, :] == expert
        turn[j : j + 1, :] = jnp.sum(jnp.where(hit, base, 0.0), axis=0, keepdims=True)
        turn[2 + j : 3 + j, :] = gate_ref[j : j + 1, :]
    turned = turn[...].T
    slot_lane = lax.broadcasted_iota(jnp.int32, (T, S * capp), 1).astype(F32)
    picks = [jnp.where(turned[:, j : j + 1] == slot_lane, 1.0, 0.0).astype(BF16) for j in range(2)]
    for i in range(1, S):
        z_return(s, lax.rem(s + i, S)).wait_recv()
    everything = ret[...].reshape(S * capp, D)
    moe_ref[...] = (
        jnp.dot(picks[0], everything, preferred_element_type=F32) * turned[:, 2:3]
        + jnp.dot(picks[1], everything, preferred_element_type=F32) * turned[:, 3:4]
    ).astype(BF16)

    def drain(i, unused):
        to = lax.rem(s + i, S)
        z_copy(to, s).wait_send()
        z_return(to, s).wait_send()
        return unused

    lax.fori_loop(1, S, drain, jnp.int32(0))

    def drain_chunk(i, unused):
        t_reduce(i).wait_send()
        for j in range(1, X):
            x_reduce(i, other_x(j), x).wait_send()

        @pl.when((i <= s) & (s + 1 < S))
        def _():
            kv_copy(i, 1).wait_send()

        @pl.when((i >= s) & (s - 1 >= 0))
        def _():
            kv_copy(i, -1).wait_send()

        return unused

    lax.fori_loop(0, S, drain_chunk, jnp.int32(0))


def fast_kernel(
    sizes,
    q_hbm, fk_hbm, fv_hbm, sk_hbm, sv_hbm, flags_hbm, tok_hbm, ids_hbm, gate_hbm,
    up_hbm, upb_hbm, down_hbm, downb_hbm,
    attn_ref, moe_ref,
    q_v, fresh_k, fresh_v, stale_k, stale_v, flags, tok_v, ids_v, gate_v,
    up_v, upb_v, down_v, downb_v,
    disp, rows, outs, tpin, xin, fin, ret, kv, keys_v, q_in, o_out, o_in, masked, acc, stat, moe, turn,
    in_sem,
    z_send, z_recv, xf_send, xf_recv, tf_send, tf_recv,
    tr_send, tr_recv, xr_send, xr_recv, zr_send, zr_recv, kv_send, kv_recv, qo_send, qo_recv,
):
    S, X, capp = sizes
    s, x, c = lax.axis_index("seq"), lax.axis_index("exp"), lax.axis_index("tp")
    oc, ox = 1 - c, 1 - x
    T, D = tok_v.shape
    W, L = q_v.shape
    heads = W // HD
    blocks = flags.shape[0]
    blk = L // blocks

    barrier = pltpu.get_barrier_semaphore()
    for i in range(1, S):
        pl.semaphore_signal(barrier, inc=1, device_id={"seq": lax.rem(s + i, S)}, device_id_type=MESH)
    pl.semaphore_signal(barrier, inc=1, device_id={"exp": ox}, device_id_type=MESH)
    pl.semaphore_signal(barrier, inc=1, device_id={"tp": oc}, device_id_type=MESH)

    pairs = (
        (ids_hbm, ids_v), (tok_hbm, tok_v), (flags_hbm, flags),
        (fk_hbm, fresh_k), (sk_hbm, stale_k), (fv_hbm, fresh_v), (sv_hbm, stale_v),
        (up_hbm.at[0], up_v), (upb_hbm, upb_v), (down_hbm.at[0], down_v), (downb_hbm, downb_v),
        (q_hbm, q_v), (gate_hbm, gate_v),
    )
    loads = [pltpu.make_async_copy(a, b, in_sem.at[i]) for i, (a, b) in enumerate(pairs)]
    for load in loads:
        load.start()

    def rdma(src, dst, ssem, rsem, where):
        return pltpu.make_async_remote_copy(
            src_ref=src, dst_ref=dst, send_sem=ssem, recv_sem=rsem,
            device_id=where, device_id_type=MESH,
        )

    def z_copy(e, slot):
        return rdma(disp.at[e], rows.at[slot, x, c], z_send.at[e], z_recv.at[slot], {"seq": e})

    def x_forward(src, origin):
        return rdma(
            rows.at[src, origin, c], rows.at[src, origin, c],
            xf_send.at[src], xf_recv.at[src], {"exp": ox},
        )

    def t_forward(src, origin, side):
        return rdma(
            rows.at[src, origin, side], rows.at[src, origin, side],
            tf_send.at[src, origin], tf_recv.at[src, origin], {"tp": oc},
        )

    def t_reduce(src, origin):
        return rdma(
            outs.at[src, origin, oc], tpin.at[src, origin],
            tr_send.at[src, origin], tr_recv.at[src, origin], {"tp": oc},
        )

    def x_reduce(src):
        return rdma(outs.at[src, ox, c], xin.at[src], xr_send.at[src], xr_recv.at[src], {"exp": ox})

    def z_return(src, slot):
        return rdma(fin.at[src], ret.at[slot], zr_send.at[src], zr_recv.at[slot], {"seq": src})

    mate, facing = s + 1 - 2 * lax.rem(s, 2), S - 1 - s
    far = S - 1 - mate
    inner = (s != 0) & (s != S - 1)

    def kv_copy(b, part, to):
        return rdma(kv.at[b, part], kv.at[b, part], kv_send.at[b, part], kv_recv.at[b, part], {"seq": to})

    def q_copy():
        return rdma(q_v, q_in, qo_send.at[0], qo_recv.at[0], {"seq": mate})

    def o_copy():
        return rdma(o_out, o_in, qo_send.at[1], qo_recv.at[1], {"seq": mate})

    def mirrored(end, inner):
        near = jnp.where((s == 0) | (s == S - 1), end, inner)
        return jnp.where(2 * s < S, near, S - 1 - near)

    targets = [mirrored(a, b) for a, b in ((1, 2), (S - 1, 0), (2, S - 1))]
    order = [s, mate, facing, far]

    loads[0].wait()
    loads[1].wait()
    expert = lax.broadcasted_iota(jnp.int32, (S, T), 0)
    named = (ids_v[0:1, :] == expert) | (ids_v[1:2, :] == expert)
    earlier = lax.broadcasted_iota(jnp.int32, (T, T), 0) < lax.broadcasted_iota(jnp.int32, (T, T), 1)
    place = jnp.dot(
        jnp.where(named, 1.0, 0.0).astype(BF16),
        jnp.where(earlier, 1.0, 0.0).astype(BF16),
        preferred_element_type=F32,
    )
    slotted = jnp.where(named, place, -1.0)
    slot_rows = lax.broadcasted_iota(jnp.int32, (capp, T), 0).astype(F32)
    for e in range(S):
        pick = jnp.where(slotted[e : e + 1, :] == slot_rows, 1.0, 0.0).astype(BF16)
        disp[e] = jnp.dot(pick, tok_v[...], preferred_element_type=F32).astype(BF16)
    rows[s, x, c] = disp[s]
    for load in loads[2:7]:
        load.wait()
    for b in range(blocks):
        fresh = flags[b] == 1
        part = pl.ds(b * blk, blk)
        kv[s, 0, :, part] = jnp.where(fresh, fresh_k[:, part], stale_k[:, part])
        kv[s, 1, :, part] = jnp.where(fresh, fresh_v[:, part], stale_v[:, part])

    pl.semaphore_wait(barrier, S - 1 + 1 + 1)

    def forward(src):
        x_forward(src, x).start()
        t_forward(src, x, c).start()

    def arrive(src):
        z_copy(src, src).wait_recv()
        forward(src)

    for e in targets:
        z_copy(e, s).start()
    forward(s)

    onward = jnp.where(inner, facing, mate)
    kv_copy(s, 0, onward).start()
    kv_copy(s, 1, onward).start()

    for load in loads[7:]:
        load.wait()

    @pl.when(jnp.logical_not(inner))
    def _():
        q_copy().start()

    scale = 1.0 / math.sqrt(HD)
    channel = lax.broadcasted_iota(jnp.int32, (W, L), 0)

    def ask(i, source):
        for h in range(heads):
            own = (channel >= h * HD) & (channel < (h + 1) * HD)
            masked[i, h] = jnp.where(own, source[...].astype(F32), 0.0).astype(BF16)

    def take(b):
        keys_v[b] = kv[b, 0].T

    def attend(i, b, first=False):
        for h in range(heads):
            lo, hi = h * HD, (h + 1) * HD
            a, z = lo // 128 * 128, min(-(-hi // 128) * 128, W)
            scores = jnp.dot(keys_v[b, :, a:z], masked[i, h, a:z, :], preferred_element_type=F32) * scale
            top = jnp.max(scores, axis=0, keepdims=True)
            if not first:
                before = stat[i, h : h + 1, :]
                top = jnp.maximum(before, top)
                fade = jnp.exp(before - top)
            probs = jnp.exp(scores - top)
            total = jnp.sum(probs, axis=0, keepdims=True)
            a, z = lo // 16 * 16, -(-hi // 16) * 16
            mixed = jnp.dot(kv[b, 1, a:z, :], probs.astype(BF16), preferred_element_type=F32)
            mixed = mixed[lo - a : hi - a]
            if not first:
                total = stat[i, heads + h : heads + h + 1, :] * fade + total
                mixed = acc[i, lo:hi, :] * fade + mixed
            stat[i, h : h + 1, :] = top
            stat[i, heads + h : heads + h + 1, :] = total
            acc[i, lo:hi, :] = mixed

    def answer(i):
        for h in range(heads):
            lo, hi = h * HD, (h + 1) * HD
            acc[i, lo:hi, :] = acc[i, lo:hi, :] / stat[i, heads + h : heads + h + 1, :]
        return acc[i].astype(BF16)

    def mlp(src, origin):
        block = rows[src, origin].reshape(2 * capp, D)
        hidden = jnp.dot(block, up_v[...], preferred_element_type=F32) + upb_v[...]
        hidden = jax.nn.gelu(hidden).astype(BF16)
        result = jnp.dot(hidden, down_v[...], preferred_element_type=F32).astype(BF16)
        outs[src, origin] = result.reshape(2, capp, D)
        t_reduce(src, origin).start()

    def mine(src):
        t_forward(src, x, oc).wait_recv()
        mlp(src, x)

    def crossed(src):
        x_forward(src, ox).wait_recv()
        t_forward(src, ox, c).start()

    def other(src):
        t_forward(src, ox, oc).wait_recv()
        mlp(src, ox)

    def reduce(src):
        t_reduce(src, ox).wait_recv()
        outs[src, ox, c] = (outs[src, ox, c].astype(F32) + tpin[src, ox].astype(F32)).astype(BF16)
        x_reduce(src).start()

    def finish(src):
        t_reduce(src, x).wait_recv()
        total = outs[src, x, c].astype(F32) + tpin[src, x].astype(F32) + downb_v[...]
        x_reduce(src).wait_recv()
        return (total + xin[src].astype(F32)).astype(BF16)

    def finish_send(src):
        fin[src] = finish(src)
        z_return(src, s).start()

    o0, o1, o2, o3 = order
    landing = [s, mate, jnp.where(inner, far, facing), jnp.where(inner, facing, far)]
    mine(o0)
    turn[...] = jnp.zeros_like(turn)
    for i, e in enumerate(landing):
        hit = [ids_v[j : j + 1, :] == e for j in range(2)]
        spot = jnp.sum(jnp.where(expert == e, place, 0.0), axis=0, keepdims=True)
        turn[i : i + 1, :] = jnp.where(hit[0] | hit[1], spot, -1.0)
        turn[S + i : S + i + 1, :] = sum(
            jnp.where(hit[j], gate_v[j : j + 1, :], 0.0) for j in range(2)
        )
    turned = turn[...].T
    slot_lane = lax.broadcasted_iota(jnp.int32, (T, capp), 1).astype(F32)

    outer = jnp.logical_not(inner)
    r1, r3 = jnp.where(inner, o1, o2), jnp.where(inner, o3, o1)

    @pl.when(inner)
    def _():
        ask(0, q_v)
        take(s)
        attend(0, s, first=True)

    arrive(o1)

    @pl.when(inner)
    def _():
        arrive(o2)

    crossed(o0)
    mine(o1)
    other(o0)
    crossed(o1)

    @pl.when(outer)
    def _():
        arrive(o2)

    other(o1)
    mine(o2)

    @pl.when(outer)
    def _():
        arrive(o3)

    crossed(o2)

    @pl.when(inner)
    def _():
        arrive(o3)
        reduce(o1)
        kv_copy(mate, 0, mate).wait_recv()
        kv_copy(mate, 0, facing).start()

    other(o2)
    mine(o3)
    reduce(o2)

    @pl.when(inner)
    def _():
        kv_copy(mate, 1, mate).wait_recv()
        kv_copy(mate, 1, facing).start()
        take(mate)

    crossed(o3)

    @pl.when(inner)
    def _():
        attend(0, mate)

    other(o3)

    @pl.when(inner)
    def _():
        q_copy().wait_recv()
        ask(1, q_in)
        attend(1, s, first=True)

    reduce(o3)

    @pl.when(outer)
    def _():
        reduce(o1)

    reduce(o0)
    finish_send(r1)

    @pl.when(inner)
    def _():
        attend(1, mate)
        kv_copy(facing, 0, facing).wait_recv()
        kv_copy(facing, 1, facing).wait_recv()
        take(facing)
        attend(1, facing)
        attend(0, facing)

    @pl.when(outer)
    def _():
        finish_send(o3)

    @pl.when(inner)
    def _():
        kv_copy(far, 0, facing).wait_recv()
        kv_copy(far, 1, facing).wait_recv()
        take(far)
        attend(1, far)
        o_out[...] = answer(1)
        o_copy().start()
        attend(0, far)
        attn_ref[...] = answer(0)

    finish_send(r3)

    @pl.when(inner & (c == 0))
    def _():
        finish_send(o2)

    def combine(i, values):
        pick = jnp.where(turned[:, i : i + 1] == slot_lane, 1.0, 0.0).astype(BF16)
        return jnp.dot(pick, values, preferred_element_type=F32) * turned[:, S + i : S + i + 1]

    moe[...] = combine(0, finish(s))

    @pl.when(inner & (c == 1))
    def _():
        finish_send(o2)

    for i in range(1, S - 1):
        z_return(s, landing[i]).wait_recv()
        moe[...] += combine(i, ret[landing[i]])

    @pl.when(jnp.logical_not(inner))
    def _():
        o_copy().wait_recv()
        attn_ref[...] = o_in[...]

    z_return(s, landing[S - 1]).wait_recv()
    moe_ref[...] = (moe[...] + combine(S - 1, ret[landing[S - 1]])).astype(BF16)

    def drain(i, unused):
        to = lax.rem(s + i, S)
        z_copy(to, s).wait_send()
        z_return(to, s).wait_send()
        return unused

    lax.fori_loop(1, S, drain, jnp.int32(0))

    def drain_chunk(i, unused):
        x_forward(i, x).wait_send()
        x_reduce(i).wait_send()
        for origin in range(X):
            t_forward(i, origin, c).wait_send()
            t_reduce(i, origin).wait_send()
        return unused

    lax.fori_loop(0, S, drain_chunk, jnp.int32(0))
    for part in range(2):
        kv_copy(s, part, onward).wait_send()

    @pl.when(inner)
    def _():
        for part in range(2):
            kv_copy(mate, part, facing).wait_send()
        o_copy().wait_send()

    @pl.when(jnp.logical_not(inner))
    def _():
        q_copy().wait_send()


def store_kernel(attn_ref, moe_ref, attn_hbm, moe_hbm, sems):
    stores = [
        pltpu.make_async_copy(attn_ref, attn_hbm, sems.at[0]),
        pltpu.make_async_copy(moe_ref, moe_hbm, sems.at[1]),
    ]
    for store in stores:
        store.start()
    for store in stores:
        store.wait()


def store(attn, moe):
    vmem = pl.BlockSpec(memory_space=pltpu.VMEM)
    hbm = pl.BlockSpec(memory_space=pltpu.HBM)
    return pl.pallas_call(
        store_kernel,
        out_shape=tuple(jax.ShapeDtypeStruct(a.shape, a.dtype) for a in (attn, moe)),
        in_specs=[vmem, vmem],
        out_specs=(hbm, hbm),
        scratch_shapes=[pltpu.SemaphoreType.DMA((2,))],
        compiler_params=pltpu.CompilerParams(vmem_limit_bytes=VMEM_LIMIT // 8),
    )(attn, moe)


def fast_call(S, X, capp, args):
    q, tok, up, flags = args[0], args[6], args[9], args[5]
    width, length = q.shape
    tokens, D = tok.shape
    hidden = up.shape[2]
    hbm = pl.BlockSpec(memory_space=pltpu.HBM)
    vmem = pl.BlockSpec(memory_space=pltpu.VMEM)
    dma = pltpu.SemaphoreType.DMA
    half = pltpu.VMEM((width, length), BF16)
    slots = pltpu.VMEM((S, capp, D), BF16)
    return pl.pallas_call(
        functools.partial(fast_kernel, (S, X, capp)),
        out_shape=(
            jax.ShapeDtypeStruct((width, length), BF16),
            jax.ShapeDtypeStruct((tokens, D), BF16),
        ),
        in_specs=[hbm] * 13,
        out_specs=(vmem, vmem),
        scratch_shapes=[
            half, half, half, half, half,
            pltpu.SMEM(flags.shape, jnp.int32),
            pltpu.VMEM((tokens, D), BF16),
            pltpu.VMEM((2, tokens), jnp.int32),
            pltpu.VMEM((2, tokens), F32),
            pltpu.VMEM((D, hidden), BF16),
            pltpu.VMEM((1, hidden), F32),
            pltpu.VMEM((hidden, D), BF16),
            pltpu.VMEM((1, D), F32),
            slots,
            pltpu.VMEM((S, X, 2, capp, D), BF16),
            pltpu.VMEM((S, X, 2, capp, D), BF16),
            pltpu.VMEM((S, X, capp, D), BF16),
            slots, slots, slots,
            pltpu.VMEM((S, 2, width, length), BF16),
            pltpu.VMEM((S, length, width), BF16),
            half, half, half,
            pltpu.VMEM((2, width // HD, width, length), BF16),
            pltpu.VMEM((2, width, length), F32),
            pltpu.VMEM((2, 2 * width // HD, length), F32),
            pltpu.VMEM((tokens, D), F32),
            pltpu.VMEM((128, tokens), F32),
            dma((13,)),
            dma((S,)), dma((S,)), dma((S,)), dma((S,)), dma((S, X)), dma((S, X)),
            dma((S, X)), dma((S, X)), dma((S,)), dma((S,)), dma((S,)), dma((S,)),
            dma((S, 2)), dma((S, 2)), dma((2,)), dma((2,)),
        ],
        compiler_params=pltpu.CompilerParams(
            collective_id=0, has_side_effects=True, vmem_limit_bytes=VMEM_LIMIT
        ),
    )(*[pltpu.with_memory_space_constraint(a, pltpu.HBM) for a in args])


def local(
    attn_query, fresh_keys, fresh_values, stale_keys, stale_values, block_flags,
    moe_tokens, expert_ids, gate_weights, up_weight, up_bias, down_weight, down_bias,
):
    S, X = lax.axis_size("seq"), lax.axis_size("exp")
    assert lax.axis_size("tp") == 2 and up_weight.shape[0] == 1
    tokens, D = moe_tokens.shape
    length, width = attn_query.shape
    hidden = up_weight.shape[2]
    cap = 5 * tokens // (2 * S)
    capp = -(-cap // 16) * 16
    if (S, X) == (4, 2):
        attn_out, moe_out = fast_call(S, X, capp, (
            attn_query.T, fresh_keys.T, fresh_values.T, stale_keys.T, stale_values.T, block_flags,
            moe_tokens, expert_ids.T, gate_weights.T,
            up_weight, up_bias, down_weight, down_bias,
        ))
        attn_out, moe_out = store(attn_out, moe_out)
        return attn_out.T, moe_out
    vmem = pl.BlockSpec(memory_space=pltpu.VMEM)
    smem = pl.BlockSpec(memory_space=pltpu.SMEM)
    hbm = pl.BlockSpec(memory_space=pl.ANY)
    dma = pltpu.SemaphoreType.DMA
    attn_out, moe_out = pl.pallas_call(
        functools.partial(layer_kernel, (S, X, capp)),
        out_shape=(
            jax.ShapeDtypeStruct((width, length), BF16),
            jax.ShapeDtypeStruct((tokens, D), BF16),
        ),
        in_specs=[vmem] * 5 + [smem] + [vmem] * 3 + [hbm, vmem, hbm, vmem],
        out_specs=(vmem, vmem),
        scratch_shapes=[
            pltpu.VMEM((D, hidden), BF16),
            pltpu.VMEM((hidden, D), BF16),
            pltpu.VMEM((S, tokens), F32),
            pltpu.VMEM((S, capp, D), BF16),
            pltpu.VMEM((S, 2, X, capp, D), BF16),
            pltpu.VMEM((S, X, capp, D), BF16),
            pltpu.VMEM((S, X, capp, D), BF16),
            pltpu.VMEM((S, capp, D), BF16),
            pltpu.VMEM((S, capp, D), BF16),
            pltpu.VMEM((S, 2, width, length), BF16),
            pltpu.VMEM((S * length, width), BF16),
            pltpu.VMEM((width, length), F32),
            pltpu.VMEM((128, tokens), F32),
            dma((2,)),
            dma((S,)), dma((S,)), dma((S, X)), dma((S, X)), dma((S, X)), dma((S, X)),
            dma((S,)), dma((S,)), dma((S, X)), dma((S, X)), dma((S,)), dma((S,)),
            dma((S,)), dma((S,)), dma((S,)),
        ],
        compiler_params=pltpu.CompilerParams(
            collective_id=0, has_side_effects=True, vmem_limit_bytes=67043328
        ),
    )(
        attn_query.T, fresh_keys.T, fresh_values.T, stale_keys.T, stale_values.T, block_flags,
        moe_tokens, expert_ids.T, gate_weights.T,
        up_weight, up_bias, down_weight, down_bias,
    )
    return attn_out.T, moe_out


def solution(mesh):
    in_specs = (
        P(("groups", "seq"), ("exp", "tp")),
        P(("groups", "seq"), ("exp", "tp")),
        P(("groups", "seq"), ("exp", "tp")),
        P(("groups", "seq"), ("exp", "tp")),
        P(("groups", "seq"), ("exp", "tp")),
        P(("groups", "seq")),
        P(("groups", "seq", "exp", "tp"), None),
        P(("groups", "seq", "exp", "tp"), None),
        P(("groups", "seq", "exp", "tp"), None),
        P("seq", None, ("exp", "tp")),
        P("seq", ("exp", "tp")),
        P("seq", ("exp", "tp"), None),
        P("seq", None),
    )
    out_specs = (P(("groups", "seq"), ("exp", "tp")), P(("groups", "seq", "exp", "tp"), None))
    return jax.shard_map(local, mesh=mesh, in_specs=in_specs, out_specs=out_specs, check_vma=False)
```
